16 devices in a mesh: dp: 2 (over y, z), tp: 8 (over x, core).
Axes of the slice: x: 4, y: 2, z: 1, core: 2. Of those that a mesh axis runs over, the one named last changes fastest.
The devices are a block of a 4x4x8 slice.
Arguments:
- x_norm: bfloat16 [8192, 1536], P(('dp', 'tp')), parts along dimension 0
- grad_y: bfloat16 [8192, 1536], P(('dp', 'tp')), parts along dimension 0
- u_gate: bfloat16 [8192, 8960], P('dp', 'tp'), parts along dimension 0
- u_up: bfloat16 [8192, 8960], P('dp', 'tp'), parts along dimension 0
- w_gate: bfloat16 [1536, 8960], P(None, 'tp')
- w_up: bfloat16 [1536, 8960], P(None, 'tp')
- w_down: bfloat16 [8960, 1536], P('tp')
- x_in: bfloat16 [8192, 1536], P(('dp', 'tp')), parts along dimension 0
- gamma: bfloat16 [1536], replicated
- grad_res: bfloat16 [8192, 1536], P(('dp', 'tp')), parts along dimension 0
- attn_out: bfloat16 [8192, 1536], P('dp', 'tp'), parts along dimension 0
- w_out: bfloat16 [1536, 1536], P('tp')
Outputs:
- output 1: bfloat16 [8192, 1536], P(('dp', 'tp')), parts along dimension 0
- output 2: bfloat16 [8192, 1536], P('dp', 'tp'), parts along dimension 0
- output 3: float32 [3072, 8960], P('dp', 'tp'), parts along dimension 0
- output 4: float32 [3072, 8960], P('dp', 'tp'), parts along dimension 0
- output 5: float32 [17920, 1536], P(('dp', 'tp')), parts along dimension 0
- output 6: float32 [3072, 1536], P(('dp', 'tp')), parts along dimension 0
There are 2 independent parts. The reference program is written for one: setup_inputs(seed, part) draws one part's arguments, and reference() takes and returns one part's arrays. A program takes and returns all parts, laid end to end along the dimension named above; an argument that names none is the same for every part.
All inputs are finite; a program needn't handle non-finite values.
Results may differ from the reference program's by a relative error of at most 0.014854.
Values are sent between devices in bfloat16 or wider.
A program may use at most 768 MiB of HBM per device.

```python
import jax
import jax.numpy as jnp
from jax import lax

HIDDEN = 1536
FFN_DIM = 8960
TOKENS = 4096
NORM_EPS = 1e-5


def setup_inputs(seed: int = 0, part: int = 0) -> dict:
    part_keys = jax.random.split(jax.random.fold_in(jax.random.key(seed), part), 7)
    weight_keys = jax.random.split(jax.random.key(seed + 1), 5)
    xin_keys = jax.random.split(part_keys[4], 2)
    act_shape = (TOKENS, HIDDEN)
    ffn_shape = (TOKENS, FFN_DIM)
    x_norm = jax.random.normal(part_keys[0], act_shape, jnp.float32)
    grad_y = jax.random.normal(part_keys[1], act_shape, jnp.float32)
    u_gate = jax.random.normal(part_keys[2], ffn_shape, jnp.float32)
    u_up = jax.random.normal(part_keys[3], ffn_shape, jnp.float32)
    xin_scale = jnp.exp(jax.random.uniform(xin_keys[0], (TOKENS, 1), jnp.float32, -1.0, 1.0))
    x_in = jax.random.normal(xin_keys[1], act_shape, jnp.float32) * xin_scale
    grad_res = 0.5 * jax.random.normal(part_keys[5], act_shape, jnp.float32)
    attn_out = jax.random.normal(part_keys[6], act_shape, jnp.float32)
    w_gate = jax.random.normal(weight_keys[0], (HIDDEN, FFN_DIM), jnp.float32) * HIDDEN ** -0.5
    w_up = jax.random.normal(weight_keys[1], (HIDDEN, FFN_DIM), jnp.float32) * HIDDEN ** -0.5
    w_down = jax.random.normal(weight_keys[2], (FFN_DIM, HIDDEN), jnp.float32) * FFN_DIM ** -0.5
    w_out = jax.random.normal(weight_keys[3], (HIDDEN, HIDDEN), jnp.float32) * HIDDEN ** -0.5
    gamma = 1.0 + 0.3 * jax.random.normal(weight_keys[4], (HIDDEN,), jnp.float32)
    return dict(
        x_norm=x_norm.astype(jnp.bfloat16),
        grad_y=grad_y.astype(jnp.bfloat16),
        u_gate=u_gate.astype(jnp.bfloat16),
        u_up=u_up.astype(jnp.bfloat16),
        w_gate=w_gate.astype(jnp.bfloat16),
        w_up=w_up.astype(jnp.bfloat16),
        w_down=w_down.astype(jnp.bfloat16),
        x_in=x_in.astype(jnp.bfloat16),
        gamma=gamma.astype(jnp.bfloat16),
        grad_res=grad_res.astype(jnp.bfloat16),
        attn_out=attn_out.astype(jnp.bfloat16),
        w_out=w_out.astype(jnp.bfloat16),
    )


def reference(x_norm, grad_y, u_gate, u_up, w_gate, w_up, w_down, x_in, gamma, grad_res, attn_out, w_out):
    gate_f = u_gate.astype(jnp.float32)
    up_f = u_up.astype(jnp.float32)
    sig_gate = jax.nn.sigmoid(gate_f)
    act_gate = gate_f * sig_gate
    silu_grad = sig_gate * (1.0 + gate_f * (1.0 - sig_gate))
    hidden_z = (act_gate * up_f).astype(jnp.bfloat16)
    gw_down = jnp.dot(hidden_z.T, grad_y, preferred_element_type=jnp.float32)
    grad_h = jnp.dot(grad_y, w_down.T, preferred_element_type=jnp.float32)
    grad_up = (grad_h * act_gate).astype(jnp.bfloat16)
    grad_gate = (grad_h * up_f * silu_grad).astype(jnp.bfloat16)
    grad_x = (jnp.dot(grad_gate, w_gate.T, preferred_element_type=jnp.float32)
              + jnp.dot(grad_up, w_up.T, preferred_element_type=jnp.float32)).astype(jnp.bfloat16)
    gw_gate = jnp.dot(x_norm.T, grad_gate, preferred_element_type=jnp.float32)
    gw_up = jnp.dot(x_norm.T, grad_up, preferred_element_type=jnp.float32)
    xin_f = x_in.astype(jnp.float32)
    inv_rms = lax.rsqrt(jnp.mean(xin_f * xin_f, axis=-1, keepdims=True) + NORM_EPS)
    scaled = grad_x.astype(jnp.float32) * gamma.astype(jnp.float32)
    proj_mean = jnp.mean(scaled * xin_f, axis=-1, keepdims=True)
    grad_sum = (grad_res.astype(jnp.float32)
                + inv_rms * (scaled - xin_f * (inv_rms * inv_rms) * proj_mean)).astype(jnp.bfloat16)
    grad_attn = jnp.dot(grad_sum, w_out.T, preferred_element_type=jnp.float32).astype(jnp.bfloat16)
    gw_out = jnp.dot(attn_out.T, grad_sum, preferred_element_type=jnp.float32)
    return grad_sum, grad_attn, gw_gate, gw_up, gw_down, gw_out
```

```python
import functools

import jax
import jax.numpy as jnp
from jax import lax
from jax.experimental import pallas as pl
from jax.experimental.pallas import tpu as pltpu
from jax.sharding import PartitionSpec as P

NORM_EPS = 1e-5
CONTRACT_ROWS = (((0,), (0,)), ((), ()))
CONTRACT_COLS = (((1,), (1,)), ((), ()))
F32, BF16 = jnp.float32, jnp.bfloat16
MESH = pl.DeviceIdType.MESH
OWN, RIGHT, LEFT, FAR = range(4)


def dot_rows(a, b):
    return lax.dot_general(a, b, CONTRACT_ROWS, preferred_element_type=F32)


def dot_cols(a, b):
    return lax.dot_general(a, b, CONTRACT_COLS, preferred_element_type=F32)


def chip_step(slot):
    return lax.rem(slot * (slot + 1) // 2, 4)


def main_kernel(n, x_hbm, gy_hbm, ug_hbm, uu_hbm, wg_hbm, wu_hbm, wd_hbm, xin_hbm, gamma_ref, gres_hbm,
                x_near, x_far, dug_near, duu_near, dug_far, duu_far, z_far, gy_far, gwg_hbm, gwu_hbm, gwd_hbm, ds_hbm,
                wg, wu, wd, buf, ug, uu, z, dug, duu, acc, prec, hop, fin,
                w_sem, u_sem, o_sem, b_sem, ys, yd, yr, xs, xd, xr, ps, pr, hs, hr, fs, fr):
    me = lax.axis_index("tp")
    core, chip, chips = lax.rem(me, 2), me // 2, n // 2
    right = lax.rem(chip + 1, chips) * 2 + core
    left = lax.rem(chip + chips - 1, chips) * 2 + core
    other = chip * 2 + 1 - core
    rows = gy_hbm.shape[0]
    half = rows // 2
    ffn = wd.shape[0]
    gy = buf
    part = 8

    def half_of(h):
        return pl.ds(h * half, half)

    def x_at(slot, h):
        if slot < 2 * FAR:
            return x_near.at[pl.ds(slot * rows + h * half, half)]
        return x_far.at[pl.ds((slot - 2 * FAR) * rows + h * half, half)]

    def remote(src, dst, send, recv, to):
        return pltpu.make_async_remote_copy(src_ref=src, dst_ref=dst, send_sem=send, recv_sem=recv,
                                            device_id={"tp": to}, device_id_type=MESH)

    def load_u(s, b):
        block = lax.rem(chip + chip_step(s // 2), chips) * 2 + lax.rem(core + lax.rem(s, 2), 2)
        cols = pl.ds(pl.multiple_of(block * rows, rows), rows)
        return (pltpu.make_async_copy(ug_hbm.at[:, cols], ug.at[b], u_sem.at[b, 0]),
                pltpu.make_async_copy(uu_hbm.at[:, cols], uu.at[b], u_sem.at[b, 1]))

    def store_near(s, b):
        cols = pl.ds(pl.multiple_of(s * rows, rows), rows)
        return (pltpu.make_async_copy(dug.at[b], dug_near.at[:, cols], o_sem.at[b, 0]),
                pltpu.make_async_copy(duu.at[b], duu_near.at[:, cols], o_sem.at[b, 1]))

    def store_far(b):
        cols = pl.ds(pl.multiple_of(b * rows, rows), rows)
        return (pltpu.make_async_copy(dug.at[b], dug_far.at[:, cols], o_sem.at[b, 0]),
                pltpu.make_async_copy(duu.at[b], duu_far.at[:, cols], o_sem.at[b, 1]),
                pltpu.make_async_copy(z.at[b], z_far.at[:, cols], o_sem.at[b, 2]))

    def store_gy(b):
        return pltpu.make_async_copy(gy.at[2 * FAR + b], gy_far.at[pl.ds(pl.multiple_of(b * rows, rows), rows)],
                                     o_sem.at[b, 3])

    def y_first(d, h):
        land = 2 * (LEFT, RIGHT)[d]
        return remote(gy_hbm.at[half_of(h)], gy.at[land, half_of(h)], ys.at[d, h], yr.at[land, h], (right, left)[d])

    def y_second(d):
        src, h = 2 * (LEFT, RIGHT)[d], d
        return remote(gy.at[src, half_of(h)], gy.at[2 * FAR, half_of(h)], ys.at[d, 2], yr.at[2 * FAR, h],
                      (right, left)[d])

    def y_swap(slot, h):
        src = gy_hbm.at[half_of(h)] if slot == OWN else gy.at[2 * slot, half_of(h)]
        return remote(src, gy.at[2 * slot + 1, half_of(h)], yd.at[slot, h], yr.at[2 * slot + 1, h], other)

    def y_own(h):
        return pltpu.make_async_copy(gy_hbm.at[half_of(h)], gy.at[0, half_of(h)], yr.at[0, h])

    def x_first(d, h):
        land = 2 * (LEFT, RIGHT)[d]
        return remote(x_hbm.at[half_of(h)], x_at(land, h), xs.at[d, h], xr.at[land, h],
                      (right, left)[d])

    def x_second(d):
        src, h = 2 * (LEFT, RIGHT)[d], d
        return remote(x_at(src, h), x_at(2 * FAR, h), xs.at[d, 2], xr.at[2 * FAR, h],
                      (right, left)[d])

    def x_swap(slot, h):
        src = x_hbm.at[half_of(h)] if slot == OWN else x_at(2 * slot, h)
        return remote(src, x_at(2 * slot + 1, h), xd.at[slot, h], xr.at[2 * slot + 1, h], other)

    x_in_copy = pltpu.make_async_copy(x_hbm, buf.at[part + FAR], b_sem.at[0])
    x_out_copy = pltpu.make_async_copy(buf.at[part + FAR], x_near.at[pl.ds(0, rows)], b_sem.at[1])

    def p_swap(slot):
        return remote(buf.at[2 * slot + 1], prec.at[slot], ps.at[slot], pr.at[slot], other)

    def r_first(d):
        return remote(buf.at[part + FAR, half_of(d)], hop.at[d], hs.at[d], hr.at[d], (right, left)[d])

    def r_last(d, h):
        src = part + (RIGHT, LEFT)[d]
        return remote(buf.at[src, half_of(h)], fin.at[d, half_of(h)], fs.at[d, h], fr.at[d, h], (right, left)[d])

    weights = [pltpu.make_async_copy(a, b, w_sem.at[i])
               for i, (a, b) in enumerate(((wd_hbm, wd), (wg_hbm, wg), (wu_hbm, wu)))]
    gw_copies = [pltpu.make_async_copy(acc, a, w_sem.at[i]) for i, a in enumerate((gwd_hbm, gwg_hbm, gwu_hbm))]

    barrier = pltpu.get_barrier_semaphore()
    for peer in (right, left, other):
        pl.semaphore_signal(barrier, inc=1, device_id={"tp": peer}, device_id_type=MESH)
    for h in (0, 1):
        y_own(h).start()
    weights[0].start()
    for c in load_u(0, 0):
        c.start()
    weights[1].start()
    weights[2].start()
    x_in_copy.start()
    pl.semaphore_wait(barrier, 3)
    for step in (0, 1):
        y_first(0, step).start()
        y_first(1, 1 - step).start()
    for h in (0, 1):
        y_swap(OWN, h).start()

    fstep = ffn // 5

    def clear():
        def body(i, carry):
            acc[pl.ds(pl.multiple_of(i * 16, 16), 16), :] = jnp.zeros((16, acc.shape[1]), F32)
            return carry

        lax.fori_loop(0, ffn // 16, body, 0)

    def accumulate(a, b):
        for f in range(5):
            lines = pl.ds(f * fstep, fstep)
            acc[lines, :] += jnp.dot(a[lines, :], b[...], preferred_element_type=F32)

    clear()
    for c in weights:
        c.wait()

    def unit(s, carry):
        slot, plane, b = s // 2, lax.rem(s, 2), lax.rem(s, 2)

        @pl.when(s + 1 < 8)
        def _():
            for c in load_u(s + 1, lax.rem(s + 1, 2)):
                c.start()

        @pl.when(s == 2)
        def _():
            y_first(0, 0).wait_recv()
            y_second(0).start()
            y_first(1, 1).wait_recv()
            y_second(1).start()
            y_swap(LEFT, 0).start()
            y_swap(RIGHT, 1).start()
            for step in (0, 1):
                x_first(0, step).start()
                x_first(1, 1 - step).start()
            x_in_copy.wait()
            x_out_copy.start()
            for k in (0, 1):
                x_swap(OWN, k).start()
            y_first(1, 0).wait_recv()
            y_swap(RIGHT, 0).start()
            y_first(0, 1).wait_recv()
            y_swap(LEFT, 1).start()

        @pl.when(s == 6)
        def _():
            x_out_copy.wait()
            for k in (0, 1):
                y_second(k).wait_recv()
                y_swap(FAR, k).start()

        @pl.when(s == 7)
        def _():
            for d in (0, 1):
                x_first(d, d).wait_recv()
                x_second(d).start()
                x_swap((LEFT, RIGHT)[d], d).start()

        @pl.when(jnp.logical_or(s == 0, plane == 1))
        def _():
            for h in (0, 1):
                pltpu.make_async_copy(gy_hbm.at[half_of(h)], gy.at[s, half_of(h)], yr.at[s, h]).wait()

        for c in load_u(s, b):
            c.wait()

        @pl.when(s >= 2)
        def _():
            for c in store_near(s - 2, b):
                c.wait()

        @pl.when(s >= 6)
        def _():
            store_gy(b).start()

        for f in range(2):
            lines = pl.ds(f * (ffn // 2), ffn // 2)
            grad_h = dot_cols(wd[lines, :], gy[s])
            gate_f = ug[b, lines, :].astype(F32)
            up_f = uu[b, lines, :].astype(F32)
            sig_gate = jax.nn.sigmoid(gate_f)
            act_gate = gate_f * sig_gate
            silu_grad = sig_gate * (1.0 + gate_f * (1.0 - sig_gate))
            z[b, lines, :] = (act_gate * up_f).astype(BF16)
            duu[b, lines, :] = (grad_h * act_gate).astype(BF16)
            dug[b, lines, :] = (grad_h * up_f * silu_grad).astype(BF16)

        @pl.when(s < 6)
        def _():
            for c in store_near(s, b):
                c.start()
            accumulate(z.at[b], gy.at[s])

        @pl.when(s >= 6)
        def _():
            for c in store_far(b):
                c.start()
            store_gy(b).wait()

        to = plane * s + (1 - plane) * (part + slot)
        for h in (0, 1):
            buf[to, half_of(h), :] = (dot_rows(dug[b, :, half_of(h)], wg[...])
                                      + dot_rows(duu[b, :, half_of(h)], wu[...])).astype(BF16)

        @pl.when(plane == 1)
        def _():
            remote(buf.at[s], prec.at[slot], ps.at[slot], pr.at[slot], other).start()

        return carry

    lax.fori_loop(0, 8, unit, 0)
    gw_copies[0].start()

    def add_into(slot, h, src, at):
        step = 64

        def body(i, carry):
            to = pl.ds(pl.multiple_of(h * half + i * step, step), step)
            frm = pl.ds(pl.multiple_of(at + i * step, step), step)
            buf[slot, to, :] = (buf[slot, to, :].astype(F32) + src[frm, :].astype(F32)).astype(BF16)
            return carry

        lax.fori_loop(0, half // step, body, 0)

    p_swap(FAR).wait_recv()
    for d in (0, 1):
        add_into(part + FAR, d, prec.at[FAR], d * half)
        r_first(d).start()
    for d, slot in ((0, RIGHT), (1, LEFT)):
        p_swap(slot).wait_recv()
        add_into(part + slot, 1 - d, prec.at[slot], (1 - d) * half)
        r_last(d, 1 - d).start()
    for d, slot in ((0, RIGHT), (1, LEFT)):
        add_into(part + slot, d, prec.at[slot], d * half)
    p_swap(OWN).wait_recv()
    for h in (0, 1):
        add_into(part + OWN, h, prec.at[OWN], h * half)
    for b in (0, 1):
        for c in store_far(b):
            c.wait()
    for d in (0, 1):
        x_first(d, 1 - d).wait_recv()
        x_swap((LEFT, RIGHT)[d], 1 - d).start()
    p_swap(OWN).wait_send()
    p_swap(RIGHT).wait_send()
    for h in (0, 1):
        for slot in range(3):
            x_swap(slot, h).wait_recv()

    def x_load(s, b):
        return pltpu.make_async_copy(x_near.at[pl.ds(pl.multiple_of(s * rows, rows), rows)], buf.at[1 + 2 * b],
                                     u_sem.at[b, 0])

    def d_load(src, s, b):
        return pltpu.make_async_copy(src.at[:, pl.ds(pl.multiple_of(s * rows, rows), rows)], dug.at[b],
                                     u_sem.at[b, 1])

    def start_loads(t):
        b = lax.rem(t, 2)
        x_load(lax.rem(t, 6), b).start()

        @pl.when(t < 6)
        def _():
            d_load(dug_near, t, b).start()

        @pl.when(t >= 6)
        def _():
            d_load(duu_near, t - 6, b).start()

    start_loads(0)
    gw_copies[0].wait()
    clear()

    def near(t, carry):
        b = lax.rem(t, 2)

        @pl.when(t + 1 < 12)
        def _():
            start_loads(t + 1)

        @pl.when(t == 6)
        def _():
            gw_copies[1].start()
            gw_copies[1].wait()
            clear()

        x_load(lax.rem(t, 6), b).wait()
        d_load(dug_near, lax.rem(t, 6), b).wait()
        accumulate(dug.at[b], buf.at[1 + 2 * b])
        return carry

    lax.fori_loop(0, 12, near, 0)
    gw_copies[2].start()

    norm_loads = (pltpu.make_async_copy(xin_hbm, buf.at[0], b_sem.at[0]),
                  pltpu.make_async_copy(gres_hbm, buf.at[1], b_sem.at[1]))
    for c in norm_loads:
        c.start()
    for d in (0, 1):
        x_second(d).wait_recv()
        x_swap(FAR, d).start()
    for d, slot in ((0, RIGHT), (1, LEFT)):
        r_first(d).wait_recv()
        add_into(part + slot, d, hop.at[d], 0)
        r_last(d, d).start()
    for c in norm_loads:
        c.wait()
    for d, h in ((0, 1), (1, 0), (0, 0), (1, 1)):
        r_last(d, h).wait_recv()

    step = 32
    gamma_f = gamma_ref[...].astype(F32)

    def norm(i, carry):
        r = pl.ds(pl.multiple_of(i * step, step), step)
        grad_x = (buf[part, r, :].astype(F32) + fin[0, r, :].astype(F32) + fin[1, r, :].astype(F32)).astype(BF16)
        xin_f = buf[0, r, :].astype(F32)
        inv_rms = lax.rsqrt(jnp.mean(xin_f * xin_f, axis=-1, keepdims=True) + NORM_EPS)
        scaled = grad_x.astype(F32) * gamma_f
        proj_mean = jnp.mean(scaled * xin_f, axis=-1, keepdims=True)
        buf[2, r, :] = (buf[1, r, :].astype(F32)
                        + inv_rms * (scaled - xin_f * (inv_rms * inv_rms) * proj_mean)).astype(BF16)
        return carry

    for h in (0, 1):
        y_swap(RIGHT, h).wait_send()
    y_second(1).wait_send()
    lax.fori_loop(0, rows // step, norm, 0)
    ds_copy = pltpu.make_async_copy(buf.at[2], ds_hbm, b_sem.at[0])
    ds_copy.start()

    for d in (0, 1):
        for h in (0, 1):
            y_first(d, h).wait_send()
            x_first(d, h).wait_send()
            r_last(d, h).wait_send()
        x_second(d).wait_send()
        r_first(d).wait_send()
    y_second(0).wait_send()
    for h in (0, 1):
        for slot in range(4):
            if slot != RIGHT:
                y_swap(slot, h).wait_send()
            x_swap(slot, h).wait_send()
        x_swap(FAR, h).wait_recv()
    for slot in (LEFT, FAR):
        p_swap(slot).wait_send()
    gw_copies[2].wait()
    ds_copy.wait()


def solution(mesh):
    n = mesh.shape["tp"]
    chips = n // 2
    right_of = [(i, ((i // 2 + 1) % chips) * 2 + i % 2) for i in range(n)]
    left_of = [(i, ((i // 2 - 1) % chips) * 2 + i % 2) for i in range(n)]
    partner_of = [(i, i ^ 1) for i in range(n)]

    def go_right(a):
        return lax.ppermute(a, "tp", right_of)

    def go_left(a):
        return lax.ppermute(a, "tp", left_of)

    def swap(a):
        return lax.ppermute(a, "tp", partner_of)

    token_spec = P(("dp", "tp"), None)
    split_cols = P("dp", "tp")
    weight_cols = P(None, "tp")
    weight_rows = P("tp", None)

    def run_main(x_norm, grad_y, u_gate_t, u_up_t, w_gate_t, w_up_t, w_down, x_in, gamma, grad_res):
        rows, hidden = x_norm.shape
        ffn, tokens = u_gate_t.shape
        half = rows // 2
        any_spec = pl.BlockSpec(memory_space=pl.ANY)
        dma = pltpu.SemaphoreType.DMA
        return pl.pallas_call(
            functools.partial(main_kernel, n),
            out_shape=[jax.ShapeDtypeStruct(*a) for a in (
                ((6 * rows, hidden), BF16), ((2 * rows, hidden), BF16),
                ((ffn, 6 * rows), BF16), ((ffn, 6 * rows), BF16), ((ffn, 2 * rows), BF16), ((ffn, 2 * rows), BF16),
                ((ffn, 2 * rows), BF16), ((2 * rows, hidden), BF16),
                ((ffn, hidden), F32), ((ffn, hidden), F32), ((ffn, hidden), F32), ((rows, hidden), BF16))],
            in_specs=[any_spec] * 8 + [pl.BlockSpec(memory_space=pltpu.VMEM), any_spec],
            out_specs=[any_spec] * 12,
            scratch_shapes=[
                pltpu.VMEM((ffn, hidden), BF16), pltpu.VMEM((ffn, hidden), BF16), pltpu.VMEM((ffn, hidden), BF16),
                pltpu.VMEM((12, rows, hidden), BF16),
                pltpu.VMEM((2, ffn, rows), BF16), pltpu.VMEM((2, ffn, rows), BF16),
                pltpu.VMEM((2, ffn, rows), BF16), pltpu.VMEM((2, ffn, rows), BF16), pltpu.VMEM((2, ffn, rows), BF16),
                pltpu.VMEM((ffn, hidden), F32), pltpu.VMEM((4, rows, hidden), BF16),
                pltpu.VMEM((2, half, hidden), BF16), pltpu.VMEM((2, rows, hidden), BF16),
                dma((3,)), dma((2, 2)), dma((2, 4)), dma((2,)),
                dma((2, 3)), dma((4, 2)), dma((8, 2)),
                dma((2, 3)), dma((4, 2)), dma((8, 2)),
                dma((4,)), dma((4,)), dma((2,)), dma((2,)), dma((2, 2)), dma((2, 2)),
            ],
            compiler_params=pltpu.CompilerParams(collective_id=0, has_side_effects=True,
                                                 vmem_limit_bytes=67_000_000),
        )(x_norm, grad_y, u_gate_t, u_up_t, w_gate_t, w_up_t, w_down, x_in, gamma.reshape(1, hidden), grad_res)

    def local_backward(x_norm, grad_y, u_gate, u_up, w_gate, w_up, w_down, x_in, gamma, grad_res, attn_out, w_out):
        me = lax.axis_index("tp")
        core, chip = me % 2, me // 2
        rows = x_norm.shape[0]
        half = rows // 2
        first_core = core == 0
        _, x_far, _, _, dug_far, duu_far, z_far, gy_far, gate_near, up_near, down_near, grad_sum = run_main(
            x_norm, grad_y, u_gate.T, u_up.T, w_gate.T, w_up.T, w_down, x_in, gamma, grad_res)

        def gather(block):
            top, low = block[:half], block[half:]
            left_top, right_low = go_right(top), go_left(low)
            left_low, right_top = go_right(low), go_left(top)
            far_top, far_low = go_right(left_top), go_left(right_low)
            halves = ((top, low), (right_top, right_low), (left_top, left_low), (far_top, far_low))
            out = []
            for pair in halves:
                mine = jnp.concatenate(pair, axis=0)
                other = swap(mine)
                out.append(jnp.concatenate(
                    [jnp.where(first_core, mine, other), jnp.where(first_core, other, mine)], axis=0))
            return out

        gs = gather(grad_sum)
        flip = (((0,), (1,)), ((), ()))
        gw_gate = gate_near.T + lax.dot_general(x_far, dug_far, flip, preferred_element_type=F32)
        gw_up = up_near.T + lax.dot_general(x_far, duu_far, flip, preferred_element_type=F32)
        gw_down = down_near + lax.dot_general(gy_far, z_far, flip, preferred_element_type=F32).T
        starts = [((chip + o) % chips) * (2 * rows) for o in (0, 1, -1, 2)]
        grad_attn = jnp.zeros(attn_out.shape, BF16)
        gw_out = None
        for i in range(4):
            piece = dot_cols(gs[i], w_out).astype(BF16)
            grad_attn = lax.dynamic_update_slice_in_dim(grad_attn, piece, starts[i], 0)
            term = dot_rows(lax.dynamic_slice_in_dim(attn_out, starts[i], 2 * rows, 0), gs[i])
            gw_out = term if gw_out is None else gw_out + term
        grad_sum = lax.dynamic_slice_in_dim(gs[0], core * rows, rows, 0)
        return grad_sum, grad_attn, gw_gate, gw_up, gw_down, gw_out

    return jax.shard_map(
        local_backward,
        mesh=mesh,
        in_specs=(token_spec, token_spec, split_cols, split_cols, weight_cols, weight_cols, weight_rows,
                  token_spec, P(None), token_spec, split_cols, weight_rows),
        out_specs=(token_spec, split_cols, split_cols, split_cols, token_spec, token_spec),
        check_vma=False,
    )
```

```python
import functools

import jax
import jax.numpy as jnp
from jax import lax
from jax.experimental import pallas as pl
from jax.experimental.pallas import tpu as pltpu
from jax.sharding import PartitionSpec as P


NORM_EPS = 1e-5
CONTRACT_ROWS = (((0,), (0,)), ((), ()))
CONTRACT_COLS = (((1,), (1,)), ((), ()))
F32, BF16 = jnp.float32, jnp.bfloat16
MESH = pl.DeviceIdType.MESH
OWN, RIGHT, LEFT, FAR = range(4)


def dot_rows(a, b):
    return lax.dot_general(a, b, CONTRACT_ROWS, preferred_element_type=F32)


def dot_cols(a, b):
    return lax.dot_general(a, b, CONTRACT_COLS, preferred_element_type=F32)


def chip_step(slot):
    return lax.rem(slot * (slot + 1) // 2, 4)


def main_kernel(n, x_hbm, gy_hbm, ug_hbm, uu_hbm, wg_hbm, wu_hbm, wd_hbm, xin_hbm, gamma_ref, gres_hbm,
                x_all, dug_all, duu_all, gwg_hbm, gwu_hbm, gwd_hbm, ds_top, ds_low, other_top, other_low, left_top, right_low,
                wg, wu, wd, buf, ug, uu, z, dug, duu, acc, prec, hop, fin,
                w_sem, u_sem, o_sem, b_sem, ys, yd, yr, xs, xd, xr, ps, pr, hs, hr, fs, fr, qs, qr, ss, sr, ds_sem,
                as_, ar):
    me = lax.axis_index("tp")
    core, chip, chips = lax.rem(me, 2), me // 2, n // 2
    right = lax.rem(chip + 1, chips) * 2 + core
    left = lax.rem(chip + chips - 1, chips) * 2 + core
    other = chip * 2 + 1 - core
    rows = gy_hbm.shape[0]
    half = rows // 2
    quarter = half // 4
    ffn = wd.shape[0]
    gy = buf
    part = 8

    def half_of(h):
        return pl.ds(h * half, half)

    def x_at(slot, h):
        return x_all.at[pl.ds(slot * rows + h * half, half)]

    def remote(src, dst, send, recv, to):
        return pltpu.make_async_remote_copy(src_ref=src, dst_ref=dst, send_sem=send, recv_sem=recv,
                                            device_id={"tp": to}, device_id_type=MESH)

    def load_u(s, b):
        block = lax.rem(chip + chip_step(s // 2), chips) * 2 + lax.rem(core + lax.rem(s, 2), 2)
        cols = pl.ds(pl.multiple_of(block * rows, rows), rows)
        return (pltpu.make_async_copy(ug_hbm.at[:, cols], ug.at[b], u_sem.at[b, 0]),
                pltpu.make_async_copy(uu_hbm.at[:, cols], uu.at[b], u_sem.at[b, 1]))

    def store_u(s, b):
        cols = pl.ds(pl.multiple_of(s * rows, rows), rows)
        return (pltpu.make_async_copy(dug.at[b], dug_all.at[:, cols], o_sem.at[b, 0]),
                pltpu.make_async_copy(duu.at[b], duu_all.at[:, cols], o_sem.at[b, 1]))

    def y_first(d, h):
        land = 2 * (LEFT, RIGHT)[d]
        return remote(gy_hbm.at[half_of(h)], gy.at[land, half_of(h)], ys.at[d, h], yr.at[land, h], (right, left)[d])

    def y_second(d):
        src, h = 2 * (LEFT, RIGHT)[d], d
        return remote(gy.at[src, half_of(h)], gy.at[2 * FAR, half_of(h)], ys.at[d, 2], yr.at[2 * FAR, h],
                      (right, left)[d])

    def y_swap(slot, h):
        src = gy_hbm.at[half_of(h)] if slot == OWN else gy.at[2 * slot, half_of(h)]
        return remote(src, gy.at[2 * slot + 1, half_of(h)], yd.at[slot, h], yr.at[2 * slot + 1, h], other)

    def y_own(h):
        return pltpu.make_async_copy(gy_hbm.at[half_of(h)], gy.at[0, half_of(h)], yr.at[0, h])

    def x_first(d, h):
        land = 2 * (LEFT, RIGHT)[d]
        return remote(x_hbm.at[half_of(h)], x_at(land, h), xs.at[d, h], xr.at[land, h],
                      (right, left)[d])

    def x_second(d):
        src, h = 2 * (LEFT, RIGHT)[d], d
        return remote(x_at(src, h), x_at(2 * FAR, h), xs.at[d, 2], xr.at[2 * FAR, h], (right, left)[d])

    def x_swap(slot, h):
        src = x_hbm.at[half_of(h)] if slot == OWN else x_at(2 * slot, h)
        return remote(src, x_at(2 * slot + 1, h), xd.at[slot, h], xr.at[2 * slot + 1, h], other)

    x_in_copy = pltpu.make_async_copy(x_hbm, buf.at[part + FAR], b_sem.at[0])
    x_out_copy = pltpu.make_async_copy(buf.at[part + FAR], x_all.at[pl.ds(0, rows)], b_sem.at[1])

    def p_swap(slot):
        return remote(buf.at[2 * slot + 1], prec.at[slot], ps.at[slot], pr.at[slot], other)

    def r_first(d):
        return remote(buf.at[part + FAR, half_of(d)], hop.at[d], hs.at[d], hr.at[d], (right, left)[d])

    def r_last(d, h):
        src = part + (RIGHT, LEFT)[d]
        return remote(buf.at[src, half_of(h)], fin.at[d, half_of(h)], fs.at[d, h], fr.at[d, h], (right, left)[d])

    def r_final(d, q):
        rws = pl.ds(d * half + q * quarter, quarter)
        return remote(buf.at[part + (RIGHT, LEFT)[d], rws], fin.at[d, rws], qs.at[d, q], qr.at[d, q],
                      (right, left)[d])

    def s_swap(h, q):
        return remote(buf.at[2, pl.ds(h * half + q * quarter, quarter)],
                      (other_top, other_low)[h].at[pl.ds(q * quarter, quarter)], ss.at[h, q], sr.at[h, q], other)

    def s_first(d, q):
        return remote(buf.at[2, pl.ds(d * half + q * quarter, quarter)],
                      (left_top, right_low)[d].at[pl.ds(q * quarter, quarter)], as_.at[d, q], ar.at[d, q],
                      (right, left)[d])

    def s_out(h, q):
        return pltpu.make_async_copy(buf.at[2, pl.ds(h * half + q * quarter, quarter)],
                                     (ds_top, ds_low)[h].at[pl.ds(q * quarter, quarter)], ds_sem.at[h, q])

    weights = [pltpu.make_async_copy(a, b, w_sem.at[i])
               for i, (a, b) in enumerate(((wd_hbm, wd), (wg_hbm, wg), (wu_hbm, wu)))]
    gw_copies = [pltpu.make_async_copy(acc, a, w_sem.at[i]) for i, a in enumerate((gwd_hbm, gwg_hbm, gwu_hbm))]

    barrier = pltpu.get_barrier_semaphore()
    for peer in (right, left, other):
        pl.semaphore_signal(barrier, inc=1, device_id={"tp": peer}, device_id_type=MESH)
    for h in (0, 1):
        y_own(h).start()
    weights[0].start()
    for c in load_u(0, 0):
        c.start()
    weights[1].start()
    weights[2].start()
    x_in_copy.start()
    pl.semaphore_wait(barrier, 3)
    for step in (0, 1):
        y_first(0, step).start()
        y_first(1, 1 - step).start()
    for h in (0, 1):
        y_swap(OWN, h).start()

    fstep = ffn // 5

    def clear():
        def body(i, carry):
            acc[pl.ds(pl.multiple_of(i * 16, 16), 16), :] = jnp.zeros((16, acc.shape[1]), F32)
            return carry

        lax.fori_loop(0, ffn // 16, body, 0)

    def accumulate(a, b):
        for f in range(5):
            lines = pl.ds(f * fstep, fstep)
            acc[lines, :] += jnp.dot(a[lines, :], b[...], preferred_element_type=F32)

    clear()
    for c in weights:
        c.wait()

    def unit(s, carry):
        slot, plane, b = s // 2, lax.rem(s, 2), lax.rem(s, 2)

        @pl.when(s + 1 < 8)
        def _():
            for c in load_u(s + 1, lax.rem(s + 1, 2)):
                c.start()

        @pl.when(s == 2)
        def _():
            y_first(0, 0).wait_recv()
            y_second(0).start()
            y_first(1, 1).wait_recv()
            y_second(1).start()
            y_swap(LEFT, 0).start()
            y_swap(RIGHT, 1).start()
            for step in (0, 1):
                x_first(0, step).start()
                x_first(1, 1 - step).start()
            x_in_copy.wait()
            x_out_copy.start()
            for k in (0, 1):
                x_swap(OWN, k).start()
            y_first(1, 0).wait_recv()
            y_swap(RIGHT, 0).start()
            y_first(0, 1).wait_recv()
            y_swap(LEFT, 1).start()

        @pl.when(s == 6)
        def _():
            x_out_copy.wait()
            for k in (0, 1):
                y_second(k).wait_recv()
                y_swap(FAR, k).start()

        @pl.when(s == 7)
        def _():
            for d in (0, 1):
                x_first(d, d).wait_recv()
                x_second(d).start()
                x_swap((LEFT, RIGHT)[d], d).start()

        @pl.when(jnp.logical_or(s == 0, plane == 1))
        def _():
            for h in (0, 1):
                pltpu.make_async_copy(gy_hbm.at[half_of(h)], gy.at[s, half_of(h)], yr.at[s, h]).wait()

        for c in load_u(s, b):
            c.wait()

        @pl.when(s >= 2)
        def _():
            for c in store_u(s - 2, b):
                c.wait()

        for f in range(2):
            lines = pl.ds(f * (ffn // 2), ffn // 2)
            grad_h = dot_cols(wd[lines, :], gy[s])
            gate_f = ug[b, lines, :].astype(F32)
            up_f = uu[b, lines, :].astype(F32)
            sig_gate = jax.nn.sigmoid(gate_f)
            act_gate = gate_f * sig_gate
            silu_grad = sig_gate * (1.0 + gate_f * (1.0 - sig_gate))
            z[lines, :] = (act_gate * up_f).astype(BF16)
            duu[b, lines, :] = (grad_h * act_gate).astype(BF16)
            dug[b, lines, :] = (grad_h * up_f * silu_grad).astype(BF16)

        for c in store_u(s, b):
            c.start()
        accumulate(z, gy.at[s])
        to = plane * s + (1 - plane) * (part + slot)
        for h in (0, 1):
            buf[to, half_of(h), :] = (dot_rows(dug[b, :, half_of(h)], wg[...])
                                      + dot_rows(duu[b, :, half_of(h)], wu[...])).astype(BF16)

        @pl.when(plane == 1)
        def _():
            remote(buf.at[s], prec.at[slot], ps.at[slot], pr.at[slot], other).start()

        return carry

    lax.fori_loop(0, 8, unit, 0)
    gw_copies[0].start()

    def add_into(slot, row, src, at, count):
        step = 64

        def body(i, carry):
            to = pl.ds(pl.multiple_of(row + i * step, step), step)
            frm = pl.ds(pl.multiple_of(at + i * step, step), step)
            buf[slot, to, :] = (buf[slot, to, :].astype(F32) + src[frm, :].astype(F32)).astype(BF16)
            return carry

        lax.fori_loop(0, count // step, body, 0)

    p_swap(FAR).wait_recv()
    for d in (0, 1):
        add_into(part + FAR, d * half, prec.at[FAR], d * half, half)
        r_first(d).start()
    for d, slot in ((0, RIGHT), (1, LEFT)):
        p_swap(slot).wait_recv()
        add_into(part + slot, (1 - d) * half, prec.at[slot], (1 - d) * half, half)
        r_last(d, 1 - d).start()
    for d, slot in ((0, RIGHT), (1, LEFT)):
        add_into(part + slot, d * half, prec.at[slot], d * half, half)
    p_swap(OWN).wait_recv()
    add_into(part + OWN, 0, prec.at[OWN], 0, rows)
    for s in (6, 7):
        for c in store_u(s, s % 2):
            c.wait()
    for d in (0, 1):
        x_first(d, 1 - d).wait_recv()
        x_swap((LEFT, RIGHT)[d], 1 - d).start()
    p_swap(OWN).wait_send()
    p_swap(RIGHT).wait_send()
    for h in (0, 1):
        for slot in range(3):
            x_swap(slot, h).wait_recv()

    def x_load(s, b):
        return pltpu.make_async_copy(x_all.at[pl.ds(pl.multiple_of(s * rows, rows), rows)], buf.at[1 + 2 * b],
                                     u_sem.at[b, 0])

    def d_load(src, s, b):
        return pltpu.make_async_copy(src.at[:, pl.ds(pl.multiple_of(s * rows, rows), rows)], dug.at[b],
                                     u_sem.at[b, 1])

    def start_loads(t):
        b = lax.rem(t, 2)
        x_load(lax.rem(t, 8), b).start()

        @pl.when(t < 8)
        def _():
            d_load(dug_all, t, b).start()

        @pl.when(t >= 8)
        def _():
            d_load(duu_all, t - 8, b).start()

    start_loads(0)
    gw_copies[0].wait()
    clear()

    def step_w(t, carry):
        b = lax.rem(t, 2)

        @pl.when(t == 5)
        def _():
            for d in (0, 1):
                x_second(d).wait_recv()
                x_swap(FAR, d).start()

        @pl.when(t == 6)
        def _():
            for h in (0, 1):
                x_swap(FAR, h).wait_recv()

        @pl.when(t + 1 < 16)
        def _():
            start_loads(t + 1)

        @pl.when(t == 8)
        def _():
            gw_copies[1].start()
            gw_copies[1].wait()
            clear()

        x_load(lax.rem(t, 8), b).wait()
        d_load(dug_all, lax.rem(t, 8), b).wait()
        accumulate(dug.at[b], buf.at[1 + 2 * b])
        return carry

    lax.fori_loop(0, 16, step_w, 0)
    gw_copies[2].start()

    norm_loads = (pltpu.make_async_copy(xin_hbm, buf.at[0], b_sem.at[0]),
                  pltpu.make_async_copy(gres_hbm, buf.at[1], b_sem.at[1]))
    for c in norm_loads:
        c.start()
    for h in (0, 1):
        y_swap(RIGHT, h).wait_send()
    y_second(1).wait_send()
    for d in (0, 1):
        r_first(d).wait_recv()
    for q in range(4):
        for d, slot in ((0, RIGHT), (1, LEFT)):
            add_into(part + slot, d * half + q * quarter, hop.at[d], q * quarter, quarter)
            r_final(d, q).start()
    for c in norm_loads:
        c.wait()
    for d in (0, 1):
        r_last(d, 1 - d).wait_recv()
    step = 32
    gamma_f = gamma_ref[...].astype(F32).reshape(1, buf.shape[2])

    def norm_rows(row):
        def norm(i, carry):
            r = pl.ds(pl.multiple_of(row + i * step, step), step)
            grad_x = (buf[part, r, :].astype(F32) + fin[0, r, :].astype(F32) + fin[1, r, :].astype(F32)).astype(BF16)
            xin_f = buf[0, r, :].astype(F32)
            inv_rms = lax.rsqrt(jnp.mean(xin_f * xin_f, axis=-1, keepdims=True) + NORM_EPS)
            scaled = grad_x.astype(F32) * gamma_f
            proj_mean = jnp.mean(scaled * xin_f, axis=-1, keepdims=True)
            buf[2, r, :] = (buf[1, r, :].astype(F32)
                            + inv_rms * (scaled - xin_f * (inv_rms * inv_rms) * proj_mean)).astype(BF16)
            return carry

        lax.fori_loop(0, quarter // step, norm, 0)

    for q in range(4):
        for h in (0, 1):
            r_final(h, q).wait_recv()
            norm_rows(h * half + q * quarter)
            s_out(h, q).start()
            s_first(h, q).start()
            s_swap(h, q).start()

    for d in (0, 1):
        for h in (0, 1):
            y_first(d, h).wait_send()
            x_first(d, h).wait_send()
        r_last(d, 1 - d).wait_send()
        x_second(d).wait_send()
        r_first(d).wait_send()
    y_second(0).wait_send()
    for h in (0, 1):
        for slot in range(4):
            if slot != RIGHT:
                y_swap(slot, h).wait_send()
            x_swap(slot, h).wait_send()
        for q in range(4):
            r_final(h, q).wait_send()
            s_swap(h, q).wait_send()
            s_swap(h, q).wait_recv()
            s_out(h, q).wait()
            s_first(h, q).wait_send()
            s_first(h, q).wait_recv()
    for slot in (LEFT, FAR):
        p_swap(slot).wait_send()
    gw_copies[2].wait()


def settle_kernel(*refs):
    held, load_sem, store_sem = refs[-3:]
    arrays = (len(refs) - 3) // 2
    slots, lines = held.shape[0], held.shape[1]
    pieces = [(a, i) for a in range(arrays) for i in range(refs[a].shape[0] // lines)]
    lag = slots // 2

    def load(k):
        a, i = pieces[k]
        return pltpu.make_async_copy(refs[a].at[pl.ds(i * lines, lines)], held.at[k % slots], load_sem.at[k % slots])

    def store(k):
        a, i = pieces[k]
        return pltpu.make_async_copy(held.at[k % slots], refs[arrays + a].at[pl.ds(i * lines, lines)],
                                     store_sem.at[k % slots])

    for k in range(slots):
        load(k).start()
    for k in range(len(pieces)):
        if k >= lag:
            store(k - lag).wait()
            if k - lag + slots < len(pieces):
                load(k - lag + slots).start()
        load(k).wait()
        store(k).start()
    for k in range(len(pieces) - lag, len(pieces)):
        store(k).wait()


def tail_kernel(n, top, low, other_top, other_low, right_top, right_low, left_top, left_low, ot_hbm, wo_hbm,
                do_hbm, gwo_hbm,
                held, ot, wo, do, gwo, l_sem, o_sem, es, er, ss, sr, qs, qr):
    me = lax.axis_index("tp")
    core, chip, chips = lax.rem(me, 2), me // 2, n // 2
    right = lax.rem(chip + 1, chips) * 2 + core
    left = lax.rem(chip + chips - 1, chips) * 2 + core
    other = chip * 2 + 1 - core
    rows = held.shape[1]
    half = rows // 2
    quarter = half // 4
    halves = {0: (top, low), 1: (other_top, other_low), 2: (right_top, right_low), 4: (left_top, left_low)}

    def half_of(h):
        return pl.ds(h * half, half)

    def remote(src, dst, send, recv, to):
        return pltpu.make_async_remote_copy(src_ref=src, dst_ref=dst, send_sem=send, recv_sem=recv,
                                            device_id={"tp": to}, device_id_type=MESH)

    def second(d, q):
        return remote((left_top, right_low)[d].at[pl.ds(q * quarter, quarter)],
                      held.at[2 * FAR, pl.ds(d * half + q * quarter, quarter)], es.at[d, q], er.at[d, q],
                      (right, left)[d])

    def swap(slot, h):
        return remote(halves[2 * slot][h], held.at[2 * slot + 1, half_of(h)], ss.at[slot - 1, h], sr.at[slot - 1, h],
                      other)

    def far_swap(h, q):
        at = pl.ds(h * half + q * quarter, quarter)
        return remote(held.at[2 * FAR, at], held.at[2 * FAR + 1, at], qs.at[h, q], qr.at[h, q], other)

    def load(block, h):
        return pltpu.make_async_copy(halves[block][h], held.at[block, half_of(h)], l_sem.at[block, h])

    ot_copy = pltpu.make_async_copy(ot_hbm, ot, l_sem.at[3, 0])
    wo_copy = pltpu.make_async_copy(wo_hbm, wo, l_sem.at[3, 1])
    gwo_copy = pltpu.make_async_copy(gwo, gwo_hbm, o_sem.at[8])

    def do_out(block):
        at = lax.rem(chip + chip_step(block // 2), chips) * 2 + lax.rem(core + block % 2, 2)
        cols = pl.ds(pl.multiple_of(at * rows, rows), rows)
        return cols, pltpu.make_async_copy(do.at[:, cols], do_hbm.at[:, cols], o_sem.at[block])

    def process(block):
        cols, out = do_out(block)
        do[:, cols] = dot_cols(wo[...], held[block]).astype(BF16)
        out.start()
        share = jnp.dot(ot[:, cols], held[block], preferred_element_type=F32)
        gwo[...] = gwo[...] + share if block else share

    barrier = pltpu.get_barrier_semaphore()
    for peer in (right, left, other):
        pl.semaphore_signal(barrier, inc=1, device_id={"tp": peer}, device_id_type=MESH)
    wo_copy.start()
    for h in (0, 1):
        load(0, h).start()
    ot_copy.start()
    for block in (1, 2, 4):
        for h in (0, 1):
            load(block, h).start()
    pl.semaphore_wait(barrier, 3)
    for q in range(4):
        for d in (0, 1):
            second(d, q).start()
    for slot in (RIGHT, LEFT):
        for h in (0, 1):
            swap(slot, h).start()
    wo_copy.wait()
    ot_copy.wait()
    for block in (0, 1, 2, 4):
        for h in (0, 1):
            load(block, h).wait()
        process(block)
    for slot in (RIGHT, LEFT):
        for h in (0, 1):
            swap(slot, h).wait_recv()
        process(2 * slot + 1)
    for q in range(4):
        for h in (0, 1):
            second(h, q).wait_recv()
            far_swap(h, q).start()
    process(2 * FAR)
    for q in range(4):
        for h in (0, 1):
            far_swap(h, q).wait_recv()
    process(2 * FAR + 1)
    gwo_copy.start()
    for q in range(4):
        for h in (0, 1):
            second(h, q).wait_send()
            far_swap(h, q).wait_send()
    for slot in (RIGHT, LEFT):
        for h in (0, 1):
            swap(slot, h).wait_send()
    for block in range(8):
        do_out(block)[1].wait()
    gwo_copy.wait()


def solution(mesh):
    n = mesh.shape["tp"]
    chips = n // 2
    right_of = [(i, ((i // 2 + 1) % chips) * 2 + i % 2) for i in range(n)]
    left_of = [(i, ((i // 2 - 1) % chips) * 2 + i % 2) for i in range(n)]

    def go_right(a):
        return lax.ppermute(a, "tp", right_of)

    def go_left(a):
        return lax.ppermute(a, "tp", left_of)

    token_spec = P(("dp", "tp"), None)
    split_cols = P("dp", "tp")
    weight_cols = P(None, "tp")
    weight_rows = P("tp", None)

    def run_main(x_norm, grad_y, u_gate_t, u_up_t, w_gate_t, w_up_t, w_down, x_in, gamma, grad_res):
        rows, hidden = x_norm.shape
        ffn, tokens = u_gate_t.shape
        half = rows // 2
        any_spec = pl.BlockSpec(memory_space=pl.ANY)
        dma = pltpu.SemaphoreType.DMA
        return pl.pallas_call(
            functools.partial(main_kernel, n),
            out_shape=[jax.ShapeDtypeStruct(*a) for a in (
                ((tokens, hidden), BF16), ((ffn, tokens), BF16), ((ffn, tokens), BF16),
                ((ffn, hidden), F32), ((ffn, hidden), F32), ((ffn, hidden), F32),
                *[((half, hidden), BF16)] * 6)],
            in_specs=[any_spec] * 8 + [pl.BlockSpec(memory_space=pltpu.VMEM), any_spec],
            out_specs=[any_spec] * 12,
            scratch_shapes=[
                pltpu.VMEM((ffn, hidden), BF16), pltpu.VMEM((ffn, hidden), BF16), pltpu.VMEM((ffn, hidden), BF16),
                pltpu.VMEM((12, rows, hidden), BF16),
                pltpu.VMEM((2, ffn, rows), BF16), pltpu.VMEM((2, ffn, rows), BF16),
                pltpu.VMEM((ffn, rows), BF16), pltpu.VMEM((2, ffn, rows), BF16), pltpu.VMEM((2, ffn, rows), BF16),
                pltpu.VMEM((ffn, hidden), F32), pltpu.VMEM((4, rows, hidden), BF16),
                pltpu.VMEM((2, half, hidden), BF16), pltpu.VMEM((2, rows, hidden), BF16),
                dma((3,)), dma((2, 2)), dma((2, 4)), dma((2,)),
                dma((2, 3)), dma((4, 2)), dma((8, 2)),
                dma((2, 3)), dma((4, 2)), dma((8, 2)),
                dma((4,)), dma((4,)), dma((2,)), dma((2,)), dma((2, 2)), dma((2, 2)),
                dma((2, 4)), dma((2, 4)), dma((2, 4)), dma((2, 4)), dma((2, 4)),
                dma((2, 4)), dma((2, 4)),
            ],
            compiler_params=pltpu.CompilerParams(collective_id=0, has_side_effects=True,
                                                 vmem_limit_bytes=67_000_000),
        )(x_norm, grad_y, u_gate_t, u_up_t, w_gate_t, w_up_t, w_down, x_in, gamma, grad_res)

    any_space = pl.BlockSpec(memory_space=pl.ANY)

    def settle(*arrays):
        lines, hidden = arrays[0].shape
        slots = 8
        return pl.pallas_call(
            settle_kernel,
            in_specs=[any_space] * len(arrays), out_specs=[any_space] * len(arrays),
            out_shape=[jax.ShapeDtypeStruct(a.shape, a.dtype) for a in arrays],
            scratch_shapes=[pltpu.VMEM((slots, lines // 5, hidden), F32), pltpu.SemaphoreType.DMA((slots,)),
                            pltpu.SemaphoreType.DMA((slots,))],
            cost_estimate=pl.CostEstimate(flops=6000 * lines * hidden, bytes_accessed=24 * lines * hidden,
                                          transcendentals=0),
        )(*arrays)

    def run_tail(halves, attn_t, w_out):
        (half, hidden), (width, tokens) = halves[0].shape, attn_t.shape
        dma = pltpu.SemaphoreType.DMA
        return pl.pallas_call(
            functools.partial(tail_kernel, n),
            in_specs=[any_space] * 10, out_specs=[any_space] * 2,
            out_shape=[jax.ShapeDtypeStruct((width, tokens), BF16), jax.ShapeDtypeStruct((width, hidden), F32)],
            scratch_shapes=[
                pltpu.VMEM((8, 2 * half, hidden), BF16), pltpu.VMEM((width, tokens), BF16),
                pltpu.VMEM((width, hidden), BF16), pltpu.VMEM((width, tokens), BF16), pltpu.VMEM((width, hidden), F32),
                dma((5, 2)), dma((9,)), dma((2, 4)), dma((2, 4)), dma((2, 2)), dma((2, 2)), dma((2, 4)), dma((2, 4))],
            compiler_params=pltpu.CompilerParams(collective_id=1, has_side_effects=True),
        )(*halves, attn_t, w_out)

    def local_backward(x_norm, grad_y, u_gate, u_up, w_gate, w_up, w_down, x_in, gamma, grad_res, attn_out, w_out):
        _, _, _, gate_t, up_t, down, top, low, other_top, other_low, left_top, right_low = run_main(
            x_norm, grad_y, u_gate.T, u_up.T, w_gate.T, w_up.T, w_down, x_in, gamma, grad_res)

        left_low = go_right(low)
        right_top = go_left(top)
        gate_t, up_t, gw_down = settle(gate_t, up_t, down)
        grad_sum = jnp.concatenate([top, low], axis=0)
        do_t, gwo = run_tail((top, low, other_top, other_low, right_top, right_low, left_top, left_low),
                             attn_out.T, w_out)
        return grad_sum, do_t.T, gate_t.T, up_t.T, gw_down, gwo

    return jax.shard_map(
        local_backward,
        mesh=mesh,
        in_specs=(token_spec, token_spec, split_cols, split_cols, weight_cols, weight_cols, weight_rows,
                  token_spec, P(None), token_spec, split_cols, weight_rows),
        out_specs=(token_spec, split_cols, split_cols, split_cols, token_spec, token_spec),
        check_vma=False,
    )
```

```python
import functools

import jax
import jax.numpy as jnp
from jax import lax
from jax.experimental import pallas as pl
from jax.experimental.pallas import tpu as pltpu
from jax.sharding import PartitionSpec as P


NORM_EPS = 1e-5
CONTRACT_ROWS = (((0,), (0,)), ((), ()))
CONTRACT_COLS = (((1,), (1,)), ((), ()))
F32, BF16 = jnp.float32, jnp.bfloat16
MESH = pl.DeviceIdType.MESH
OWN, RIGHT, LEFT, FAR = range(4)


def dot_rows(a, b):
    return lax.dot_general(a, b, CONTRACT_ROWS, preferred_element_type=F32)


def dot_cols(a, b):
    return lax.dot_general(a, b, CONTRACT_COLS, preferred_element_type=F32)


def chip_step(slot):
    return lax.rem(slot * (slot + 1) // 2, 4)


def main_kernel(n, x_hbm, gy_hbm, ug_hbm, uu_hbm, wg_hbm, wu_hbm, wd_hbm, xin_hbm, gamma_ref, gres_hbm,
                x_all, dug_all, duu_all, gwg_hbm, gwu_hbm, gwd_hbm, ds_top, ds_low, other_top, other_low, left_top, right_low,
                wg, wu, wd, buf, ug, uu, z, dug, duu, acc, prec, hop, fin,
                w_sem, u_sem, o_sem, b_sem, ys, yd, yr, xs, xd, xr, ps, pr, hs, hr, fs, fr, qs, qr, ss, sr, ds_sem,
                as_, ar):
    me = lax.axis_index("tp")
    core, chip, chips = lax.rem(me, 2), me // 2, n // 2
    right = lax.rem(chip + 1, chips) * 2 + core
    left = lax.rem(chip + chips - 1, chips) * 2 + core
    other = chip * 2 + 1 - core
    rows = gy_hbm.shape[0]
    half = rows // 2
    quarter = half // 4
    ffn = wd.shape[0]
    gy = buf
    part = 8

    def half_of(h):
        return pl.ds(h * half, half)

    def x_at(slot, h):
        return x_all.at[pl.ds(slot * rows + h * half, half)]

    def remote(src, dst, send, recv, to):
        return pltpu.make_async_remote_copy(src_ref=src, dst_ref=dst, send_sem=send, recv_sem=recv,
                                            device_id={"tp": to}, device_id_type=MESH)

    def load_u(s, b):
        block = lax.rem(chip + chip_step(s // 2), chips) * 2 + lax.rem(core + lax.rem(s, 2), 2)
        cols = pl.ds(pl.multiple_of(block * rows, rows), rows)
        return (pltpu.make_async_copy(ug_hbm.at[:, cols], ug.at[b], u_sem.at[b, 0]),
                pltpu.make_async_copy(uu_hbm.at[:, cols], uu.at[b], u_sem.at[b, 1]))

    def store_u(s, b):
        cols = pl.ds(pl.multiple_of(s * rows, rows), rows)
        return (pltpu.make_async_copy(dug.at[b], dug_all.at[:, cols], o_sem.at[b, 0]),
                pltpu.make_async_copy(duu.at[b], duu_all.at[:, cols], o_sem.at[b, 1]))

    def y_first(d, h):
        land = 2 * (LEFT, RIGHT)[d]
        return remote(gy_hbm.at[half_of(h)], gy.at[land, half_of(h)], ys.at[d, h], yr.at[land, h], (right, left)[d])

    def y_second(d):
        src, h = 2 * (LEFT, RIGHT)[d], d
        return remote(gy.at[src, half_of(h)], gy.at[2 * FAR, half_of(h)], ys.at[d, 2], yr.at[2 * FAR, h],
                      (right, left)[d])

    def y_swap(slot, h):
        src = gy_hbm.at[half_of(h)] if slot == OWN else gy.at[2 * slot, half_of(h)]
        return remote(src, gy.at[2 * slot + 1, half_of(h)], yd.at[slot, h], yr.at[2 * slot + 1, h], other)

    def y_own(h):
        return pltpu.make_async_copy(gy_hbm.at[half_of(h)], gy.at[0, half_of(h)], yr.at[0, h])

    def x_first(d, h):
        land = 2 * (LEFT, RIGHT)[d]
        return remote(x_hbm.at[half_of(h)], x_at(land, h), xs.at[d, h], xr.at[land, h],
                      (right, left)[d])

    def x_second(d):
        src, h = 2 * (LEFT, RIGHT)[d], d
        return remote(x_at(src, h), x_at(2 * FAR, h), xs.at[d, 2], xr.at[2 * FAR, h], (right, left)[d])

    def x_swap(slot, h):
        src = x_hbm.at[half_of(h)] if slot == OWN else x_at(2 * slot, h)
        return remote(src, x_at(2 * slot + 1, h), xd.at[slot, h], xr.at[2 * slot + 1, h], other)

    x_in_copy = pltpu.make_async_copy(x_hbm, buf.at[part + FAR], b_sem.at[0])
    x_out_copy = pltpu.make_async_copy(buf.at[part + FAR], x_all.at[pl.ds(0, rows)], b_sem.at[1])

    def p_swap(slot):
        return remote(buf.at[2 * slot + 1], prec.at[slot], ps.at[slot], pr.at[slot], other)

    def r_first(d):
        return remote(buf.at[part + FAR, half_of(d)], hop.at[d], hs.at[d], hr.at[d], (right, left)[d])

    def r_last(d, h):
        src = part + (RIGHT, LEFT)[d]
        return remote(buf.at[src, half_of(h)], fin.at[d, half_of(h)], fs.at[d, h], fr.at[d, h], (right, left)[d])

    def r_final(d, q):
        rws = pl.ds(d * half + q * quarter, quarter)
        return remote(buf.at[part + (RIGHT, LEFT)[d], rws], fin.at[d, rws], qs.at[d, q], qr.at[d, q],
                      (right, left)[d])

    def s_swap(h, q):
        return remote(buf.at[2, pl.ds(h * half + q * quarter, quarter)],
                      (other_top, other_low)[h].at[pl.ds(q * quarter, quarter)], ss.at[h, q], sr.at[h, q], other)

    def s_first(d, q):
        return remote(buf.at[2, pl.ds(d * half + q * quarter, quarter)],
                      (left_top, right_low)[d].at[pl.ds(q * quarter, quarter)], as_.at[d, q], ar.at[d, q],
                      (right, left)[d])

    def s_out(h, q):
        return pltpu.make_async_copy(buf.at[2, pl.ds(h * half + q * quarter, quarter)],
                                     (ds_top, ds_low)[h].at[pl.ds(q * quarter, quarter)], ds_sem.at[h, q])

    weights = [pltpu.make_async_copy(a, b, w_sem.at[i])
               for i, (a, b) in enumerate(((wd_hbm, wd), (wg_hbm, wg), (wu_hbm, wu)))]
    gw_copies = [pltpu.make_async_copy(acc, a, w_sem.at[i]) for i, a in enumerate((gwd_hbm, gwg_hbm, gwu_hbm))]

    barrier = pltpu.get_barrier_semaphore()
    for peer in (right, left, other):
        pl.semaphore_signal(barrier, inc=1, device_id={"tp": peer}, device_id_type=MESH)
    for h in (0, 1):
        y_own(h).start()
    weights[0].start()
    for c in load_u(0, 0):
        c.start()
    weights[1].start()
    weights[2].start()
    x_in_copy.start()
    pl.semaphore_wait(barrier, 3)
    for step in (0, 1):
        y_first(0, step).start()
        y_first(1, 1 - step).start()
    for h in (0, 1):
        y_swap(OWN, h).start()

    fstep = ffn // 5

    def clear():
        def body(i, carry):
            acc[pl.ds(pl.multiple_of(i * 16, 16), 16), :] = jnp.zeros((16, acc.shape[1]), F32)
            return carry

        lax.fori_loop(0, ffn // 16, body, 0)

    def accumulate(a, b):
        for f in range(5):
            lines = pl.ds(f * fstep, fstep)
            acc[lines, :] += jnp.dot(a[lines, :], b[...], preferred_element_type=F32)

    clear()
    for c in weights:
        c.wait()

    def unit(s, carry):
        slot, plane, b = s // 2, lax.rem(s, 2), lax.rem(s, 2)

        @pl.when(s + 1 < 8)
        def _():
            for c in load_u(s + 1, lax.rem(s + 1, 2)):
                c.start()

        @pl.when(s == 2)
        def _():
            y_first(0, 0).wait_recv()
            y_second(0).start()
            y_first(1, 1).wait_recv()
            y_second(1).start()
            y_swap(LEFT, 0).start()
            y_swap(RIGHT, 1).start()
            for step in (0, 1):
                x_first(0, step).start()
                x_first(1, 1 - step).start()
            x_in_copy.wait()
            x_out_copy.start()
            for k in (0, 1):
                x_swap(OWN, k).start()
            y_first(1, 0).wait_recv()
            y_swap(RIGHT, 0).start()
            y_first(0, 1).wait_recv()
            y_swap(LEFT, 1).start()

        @pl.when(s == 6)
        def _():
            x_out_copy.wait()
            for k in (0, 1):
                y_second(k).wait_recv()
                y_swap(FAR, k).start()

        @pl.when(s == 7)
        def _():
            for d in (0, 1):
                x_first(d, d).wait_recv()
                x_second(d).start()
                x_swap((LEFT, RIGHT)[d], d).start()

        @pl.when(jnp.logical_or(s == 0, plane == 1))
        def _():
            for h in (0, 1):
                pltpu.make_async_copy(gy_hbm.at[half_of(h)], gy.at[s, half_of(h)], yr.at[s, h]).wait()

        for c in load_u(s, b):
            c.wait()

        @pl.when(s >= 2)
        def _():
            for c in store_u(s - 2, b):
                c.wait()

        for f in range(2):
            lines = pl.ds(f * (ffn // 2), ffn // 2)
            grad_h = dot_cols(wd[lines, :], gy[s])
            gate_f = ug[b, lines, :].astype(F32)
            up_f = uu[b, lines, :].astype(F32)
            sig_gate = jax.nn.sigmoid(gate_f)
            act_gate = gate_f * sig_gate
            silu_grad = sig_gate * (1.0 + gate_f * (1.0 - sig_gate))
            z[lines, :] = (act_gate * up_f).astype(BF16)
            duu[b, lines, :] = (grad_h * act_gate).astype(BF16)
            dug[b, lines, :] = (grad_h * up_f * silu_grad).astype(BF16)

        for c in store_u(s, b):
            c.start()
        accumulate(z, gy.at[s])
        to = plane * s + (1 - plane) * (part + slot)
        for h in (0, 1):
            buf[to, half_of(h), :] = (dot_rows(dug[b, :, half_of(h)], wg[...])
                                      + dot_rows(duu[b, :, half_of(h)], wu[...])).astype(BF16)

        @pl.when(plane == 1)
        def _():
            remote(buf.at[s], prec.at[slot], ps.at[slot], pr.at[slot], other).start()

        return carry

    lax.fori_loop(0, 8, unit, 0)
    gw_copies[0].start()

    def add_into(slot, row, src, at, count):
        step = 64

        def body(i, carry):
            to = pl.ds(pl.multiple_of(row + i * step, step), step)
            frm = pl.ds(pl.multiple_of(at + i * step, step), step)
            buf[slot, to, :] = (buf[slot, to, :].astype(F32) + src[frm, :].astype(F32)).astype(BF16)
            return carry

        lax.fori_loop(0, count // step, body, 0)

    p_swap(FAR).wait_recv()
    for d in (0, 1):
        add_into(part + FAR, d * half, prec.at[FAR], d * half, half)
        r_first(d).start()
    for d, slot in ((0, RIGHT), (1, LEFT)):
        p_swap(slot).wait_recv()
        add_into(part + slot, (1 - d) * half, prec.at[slot], (1 - d) * half, half)
        r_last(d, 1 - d).start()
    for d, slot in ((0, RIGHT), (1, LEFT)):
        add_into(part + slot, d * half, prec.at[slot], d * half, half)
    p_swap(OWN).wait_recv()
    add_into(part + OWN, 0, prec.at[OWN], 0, rows)
    for s in (6, 7):
        for c in store_u(s, s % 2):
            c.wait()
    for d in (0, 1):
        x_first(d, 1 - d).wait_recv()
        x_swap((LEFT, RIGHT)[d], 1 - d).start()
    p_swap(OWN).wait_send()
    p_swap(RIGHT).wait_send()
    for h in (0, 1):
        for slot in range(3):
            x_swap(slot, h).wait_recv()

    def x_load(s, b):
        return pltpu.make_async_copy(x_all.at[pl.ds(pl.multiple_of(s * rows, rows), rows)], buf.at[1 + 2 * b],
                                     u_sem.at[b, 0])

    def d_load(src, s, b):
        return pltpu.make_async_copy(src.at[:, pl.ds(pl.multiple_of(s * rows, rows), rows)], dug.at[b],
                                     u_sem.at[b, 1])

    def start_loads(t):
        b = lax.rem(t, 2)
        x_load(lax.rem(t, 8), b).start()

        @pl.when(t < 8)
        def _():
            d_load(dug_all, t, b).start()

        @pl.when(t >= 8)
        def _():
            d_load(duu_all, t - 8, b).start()

    start_loads(0)
    gw_copies[0].wait()
    clear()

    def step_w(t, carry):
        b = lax.rem(t, 2)

        @pl.when(t == 5)
        def _():
            for d in (0, 1):
                x_second(d).wait_recv()
                x_swap(FAR, d).start()

        @pl.when(t == 6)
        def _():
            for h in (0, 1):
                x_swap(FAR, h).wait_recv()

        @pl.when(t + 1 < 16)
        def _():
            start_loads(t + 1)

        @pl.when(t == 8)
        def _():
            gw_copies[1].start()
            gw_copies[1].wait()
            clear()

        x_load(lax.rem(t, 8), b).wait()
        d_load(dug_all, lax.rem(t, 8), b).wait()
        accumulate(dug.at[b], buf.at[1 + 2 * b])
        return carry

    lax.fori_loop(0, 16, step_w, 0)
    gw_copies[2].start()

    norm_loads = (pltpu.make_async_copy(xin_hbm, buf.at[0], b_sem.at[0]),
                  pltpu.make_async_copy(gres_hbm, buf.at[1], b_sem.at[1]))
    for c in norm_loads:
        c.start()
    for h in (0, 1):
        y_swap(RIGHT, h).wait_send()
    y_second(1).wait_send()
    for d in (0, 1):
        r_first(d).wait_recv()
    for q in range(4):
        for d, slot in ((0, RIGHT), (1, LEFT)):
            add_into(part + slot, d * half + q * quarter, hop.at[d], q * quarter, quarter)
            r_final(d, q).start()
    for c in norm_loads:
        c.wait()
    for d in (0, 1):
        r_last(d, 1 - d).wait_recv()
    step = 32
    gamma_f = gamma_ref[...].astype(F32).reshape(1, buf.shape[2])

    def norm_rows(row):
        def norm(i, carry):
            r = pl.ds(pl.multiple_of(row + i * step, step), step)
            grad_x = (buf[part, r, :].astype(F32) + fin[0, r, :].astype(F32) + fin[1, r, :].astype(F32)).astype(BF16)
            xin_f = buf[0, r, :].astype(F32)
            inv_rms = lax.rsqrt(jnp.mean(xin_f * xin_f, axis=-1, keepdims=True) + NORM_EPS)
            scaled = grad_x.astype(F32) * gamma_f
            proj_mean = jnp.mean(scaled * xin_f, axis=-1, keepdims=True)
            buf[2, r, :] = (buf[1, r, :].astype(F32)
                            + inv_rms * (scaled - xin_f * (inv_rms * inv_rms) * proj_mean)).astype(BF16)
            return carry

        lax.fori_loop(0, quarter // step, norm, 0)

    for q in range(4):
        for h in (0, 1):
            r_final(h, q).wait_recv()
            norm_rows(h * half + q * quarter)
            s_out(h, q).start()
            s_first(h, q).start()
            s_swap(h, q).start()

    for d in (0, 1):
        for h in (0, 1):
            y_first(d, h).wait_send()
            x_first(d, h).wait_send()
        r_last(d, 1 - d).wait_send()
        x_second(d).wait_send()
        r_first(d).wait_send()
    y_second(0).wait_send()
    for h in (0, 1):
        for slot in range(4):
            if slot != RIGHT:
                y_swap(slot, h).wait_send()
            x_swap(slot, h).wait_send()
        for q in range(4):
            r_final(h, q).wait_send()
            s_swap(h, q).wait_send()
            s_swap(h, q).wait_recv()
            s_out(h, q).wait()
            s_first(h, q).wait_send()
            s_first(h, q).wait_recv()
    for slot in (LEFT, FAR):
        p_swap(slot).wait_send()
    gw_copies[2].wait()


def settle_kernel(*refs):
    held, load_sem, store_sem = refs[-3:]
    arrays = (len(refs) - 3) // 2
    slots, lines = held.shape[0], held.shape[1]
    pieces = [(a, i) for a in range(arrays) for i in range(refs[a].shape[0] // lines)]
    lag = slots // 2

    def load(k):
        a, i = pieces[k]
        return pltpu.make_async_copy(refs[a].at[pl.ds(i * lines, lines)], held.at[k % slots], load_sem.at[k % slots])

    def store(k):
        a, i = pieces[k]
        return pltpu.make_async_copy(held.at[k % slots], refs[arrays + a].at[pl.ds(i * lines, lines)],
                                     store_sem.at[k % slots])

    for k in range(slots):
        load(k).start()
    for k in range(len(pieces)):
        if k >= lag:
            store(k - lag).wait()
            if k - lag + slots < len(pieces):
                load(k - lag + slots).start()
        load(k).wait()
        store(k).start()
    for k in range(len(pieces) - lag, len(pieces)):
        store(k).wait()


def attn_kernel(n, slots, *refs):
    chunks = len(slots)
    halves = refs[:4 * chunks]
    held, ot, wo, do, gwo, h_sem, l_sem, o_sem = refs[-8:]
    rest = refs[4 * chunks:-8]
    ot_hbm, wo_hbm = rest[:2]
    do_hbm, gwo_hbm = rest[-2:]
    me = lax.axis_index("tp")
    core, chip, chips = lax.rem(me, 2), me // 2, n // 2
    rows = held.shape[1]
    half = rows // 2
    loads = [pltpu.make_async_copy(src, held.at[k // 2, pl.ds(k % 2 * half, half)], h_sem.at[k])
             for k, src in enumerate(halves)]

    def place(block):
        there = lax.rem(chip + chip_step(slots[block // 2]), chips) * 2 + lax.rem(core + block % 2, 2)
        return pl.ds(pl.multiple_of(there * rows, rows), rows)

    wo_load = pltpu.make_async_copy(wo_hbm, wo, l_sem.at[0])
    gwo_load = None if slots[0] == OWN else pltpu.make_async_copy(rest[2], gwo, l_sem.at[1])
    ots = [pltpu.make_async_copy(ot_hbm.at[:, place(b)], ot.at[b], l_sem.at[2 + b]) for b in range(2 * chunks)]
    wo_load.start()
    for b in range(2 * chunks):
        loads[2 * b].start()
        loads[2 * b + 1].start()
        ots[b].start()
        if b == 0 and gwo_load is not None:
            gwo_load.start()
    wo_load.wait()
    outs = []
    for b in range(2 * chunks):
        loads[2 * b].wait()
        loads[2 * b + 1].wait()
        if slots[0] == OWN and b == 0:
            outs.append(pltpu.make_async_copy(held.at[0], rest[2], o_sem.at[2 * chunks + 1]))
            outs[-1].start()
        do[b] = dot_cols(wo[...], held[b]).astype(BF16)
        outs.append(pltpu.make_async_copy(do.at[b], do_hbm.at[:, place(b)], o_sem.at[b]))
        outs[-1].start()
        ots[b].wait()
        if b == 0 and gwo_load is not None:
            gwo_load.wait()
        share = jnp.dot(ot[b], held[b], preferred_element_type=F32)
        gwo[...] = share if slots[b // 2] == OWN and b == 0 else gwo[...] + share
    outs.append(pltpu.make_async_copy(gwo, gwo_hbm, o_sem.at[2 * chunks]))
    outs[-1].start()
    for c in outs:
        c.wait()


def solution(mesh):
    n = mesh.shape["tp"]
    chips = n // 2
    right_of = [(i, ((i // 2 + 1) % chips) * 2 + i % 2) for i in range(n)]
    partner_of = [(i, i ^ 1) for i in range(n)]
    left_of = [(i, ((i // 2 - 1) % chips) * 2 + i % 2) for i in range(n)]

    def go_right(a):
        return lax.ppermute(a, "tp", right_of)

    def go_left(a):
        return lax.ppermute(a, "tp", left_of)

    def swap(a):
        return lax.ppermute(a, "tp", partner_of)

    token_spec = P(("dp", "tp"), None)
    split_cols = P("dp", "tp")
    weight_cols = P(None, "tp")
    weight_rows = P("tp", None)

    def run_main(x_norm, grad_y, u_gate_t, u_up_t, w_gate_t, w_up_t, w_down, x_in, gamma, grad_res):
        rows, hidden = x_norm.shape
        ffn, tokens = u_gate_t.shape
        half = rows // 2
        any_spec = pl.BlockSpec(memory_space=pl.ANY)
        dma = pltpu.SemaphoreType.DMA
        return pl.pallas_call(
            functools.partial(main_kernel, n),
            out_shape=[jax.ShapeDtypeStruct(*a) for a in (
                ((tokens, hidden), BF16), ((ffn, tokens), BF16), ((ffn, tokens), BF16),
                ((ffn, hidden), F32), ((ffn, hidden), F32), ((ffn, hidden), F32),
                *[((half, hidden), BF16)] * 6)],
            in_specs=[any_spec] * 8 + [pl.BlockSpec(memory_space=pltpu.VMEM), any_spec],
            out_specs=[any_spec] * 12,
            scratch_shapes=[
                pltpu.VMEM((ffn, hidden), BF16), pltpu.VMEM((ffn, hidden), BF16), pltpu.VMEM((ffn, hidden), BF16),
                pltpu.VMEM((12, rows, hidden), BF16),
                pltpu.VMEM((2, ffn, rows), BF16), pltpu.VMEM((2, ffn, rows), BF16),
                pltpu.VMEM((ffn, rows), BF16), pltpu.VMEM((2, ffn, rows), BF16), pltpu.VMEM((2, ffn, rows), BF16),
                pltpu.VMEM((ffn, hidden), F32), pltpu.VMEM((4, rows, hidden), BF16),
                pltpu.VMEM((2, half, hidden), BF16), pltpu.VMEM((2, rows, hidden), BF16),
                dma((3,)), dma((2, 2)), dma((2, 4)), dma((2,)),
                dma((2, 3)), dma((4, 2)), dma((8, 2)),
                dma((2, 3)), dma((4, 2)), dma((8, 2)),
                dma((4,)), dma((4,)), dma((2,)), dma((2,)), dma((2, 2)), dma((2, 2)),
                dma((2, 4)), dma((2, 4)), dma((2, 4)), dma((2, 4)), dma((2, 4)),
                dma((2, 4)), dma((2, 4)),
            ],
            compiler_params=pltpu.CompilerParams(collective_id=0, has_side_effects=True,
                                                 vmem_limit_bytes=67_000_000),
        )(x_norm, grad_y, u_gate_t, u_up_t, w_gate_t, w_up_t, w_down, x_in, gamma, grad_res)

    any_space = pl.BlockSpec(memory_space=pl.ANY)

    def settle(*arrays):
        lines, hidden = arrays[0].shape
        slots = min(16, 10 * len(arrays))
        return pl.pallas_call(
            settle_kernel,
            in_specs=[any_space] * len(arrays), out_specs=[any_space] * len(arrays),
            out_shape=[jax.ShapeDtypeStruct(a.shape, a.dtype) for a in arrays],
            scratch_shapes=[pltpu.VMEM((slots, lines // 10, hidden), F32), pltpu.SemaphoreType.DMA((slots,)),
                            pltpu.SemaphoreType.DMA((slots,))],
            cost_estimate=pl.CostEstimate(flops=2000 * len(arrays) * lines * hidden,
                                          bytes_accessed=8 * len(arrays) * lines * hidden, transcendentals=0),
            compiler_params=pltpu.CompilerParams(vmem_limit_bytes=67_000_000),
        )(*arrays)

    def attn(slots, halves, attn_t, w_out, *sofar):
        (half, hidden), (width, tokens) = halves[0].shape, attn_t.shape
        blocks = 2 * len(slots)
        dma = pltpu.SemaphoreType.DMA
        results = [jax.ShapeDtypeStruct((width, tokens), BF16), jax.ShapeDtypeStruct((width, hidden), F32)]
        if not sofar:
            results.insert(0, jax.ShapeDtypeStruct((2 * half, hidden), BF16))
        return pl.pallas_call(
            functools.partial(attn_kernel, n, slots),
            in_specs=[any_space] * (2 * blocks + 2 + len(sofar)), out_specs=[any_space] * len(results),
            scratch_shapes=[
                pltpu.VMEM((blocks, 2 * half, hidden), BF16), pltpu.VMEM((blocks, width, 2 * half), BF16),
                pltpu.VMEM((width, hidden), BF16), pltpu.VMEM((blocks, width, 2 * half), BF16),
                pltpu.VMEM((width, hidden), F32), dma((2 * blocks,)), dma((2 + blocks,)), dma((2 + blocks,))],
            out_shape=results,
            input_output_aliases={2 * blocks + 3: 0} if sofar else {},
            cost_estimate=pl.CostEstimate(flops=600 * blocks * half * hidden, bytes_accessed=8 * blocks * half * hidden,
                                          transcendentals=0),
            compiler_params=pltpu.CompilerParams(vmem_limit_bytes=67_000_000),
        )(*halves, attn_t, w_out, *sofar)

    def local_backward(x_norm, grad_y, u_gate, u_up, w_gate, w_up, w_down, x_in, gamma, grad_res, attn_out, w_out):
        attn_t = attn_out.T
        _, _, _, gate_t, up_t, down, top, low, other_top, other_low, left_top, right_low = run_main(
            x_norm, grad_y, u_gate.T, u_up.T, w_gate.T, w_up.T, w_down, x_in, gamma, grad_res)

        left_low = go_right(low)
        right_top = go_left(top)
        left_top_other, right_low_other = swap(left_top), swap(right_low)
        gate_t, up_t = settle(gate_t, up_t)
        far_top = go_right(left_top)
        far_low = go_left(right_low)
        grad_sum, do_t, gwo = attn((OWN,), (top, low, other_top, other_low), attn_t, w_out)
        left_low_other, right_top_other = swap(left_low), swap(right_top)
        gw_down, = settle(down)
        do_t, gwo = attn((RIGHT, LEFT), (
            right_top, right_low, right_top_other, right_low_other,
            left_top, left_low, left_top_other, left_low_other), attn_t, w_out, gwo, do_t)
        far = (far_top, far_low, swap(far_top), swap(far_low))
        do_t, gwo = attn((FAR,), far, attn_t, w_out, gwo, do_t)
        return grad_sum, do_t.T, gate_t.T, up_t.T, gw_down, gwo

    return jax.shard_map(
        local_backward,
        mesh=mesh,
        in_specs=(token_spec, token_spec, split_cols, split_cols, weight_cols, weight_cols, weight_rows,
                  token_spec, P(None), token_spec, split_cols, weight_rows),
        out_specs=(token_spec, split_cols, split_cols, split_cols, token_spec, token_spec),
        check_vma=False,
    )
```

```python
import functools

import jax
import jax.numpy as jnp
from jax import lax
from jax.experimental import pallas as pl
from jax.experimental.pallas import tpu as pltpu
from jax.sharding import PartitionSpec as P


NORM_EPS = 1e-5
CONTRACT_ROWS = (((0,), (0,)), ((), ()))
CONTRACT_COLS = (((1,), (1,)), ((), ()))
F32, BF16 = jnp.float32, jnp.bfloat16
MESH = pl.DeviceIdType.MESH
OWN, RIGHT, LEFT, FAR = range(4)


def dot_rows(a, b):
    return lax.dot_general(a, b, CONTRACT_ROWS, preferred_element_type=F32)


def dot_cols(a, b):
    return lax.dot_general(a, b, CONTRACT_COLS, preferred_element_type=F32)


def chip_step(slot):
    return lax.rem(slot * (slot + 1) // 2, 4)


def main_kernel(n, x_hbm, gy_hbm, ug_hbm, uu_hbm, wg_hbm, wu_hbm, wd_hbm, xin_hbm, gamma_ref, gres_hbm,
                x_all, dug_all, duu_all, gwg_hbm, gwu_hbm, gwd_hbm, ds_top_a, ds_top_b, ds_low_a, ds_low_b,
                other_top, other_low, left_top, right_low,
                wg, wu, wd, buf, ug, uu, z, dug, duu, acc, prec, hop, fin,
                w_sem, u_sem, o_sem, b_sem, ys, yd, yr, xs, xd, xr, ps, pr, hs, hr, fs, fr, qs, qr, ss, sr, ds_sem,
                as_, ar):
    me = lax.axis_index("tp")
    core, chip, chips = lax.rem(me, 2), me // 2, n // 2
    right = lax.rem(chip + 1, chips) * 2 + core
    left = lax.rem(chip + chips - 1, chips) * 2 + core
    other = chip * 2 + 1 - core
    rows = gy_hbm.shape[0]
    half = rows // 2
    quarter = half // 4
    ffn = wd.shape[0]
    gy = buf
    part = 8

    def half_of(h):
        return pl.ds(h * half, half)

    def x_at(slot, h):
        return x_all.at[pl.ds(slot * rows + h * half, half)]

    def remote(src, dst, send, recv, to):
        return pltpu.make_async_remote_copy(src_ref=src, dst_ref=dst, send_sem=send, recv_sem=recv,
                                            device_id={"tp": to}, device_id_type=MESH)

    def load_u(s, b):
        block = lax.rem(chip + chip_step(s // 2), chips) * 2 + lax.rem(core + lax.rem(s, 2), 2)
        cols = pl.ds(pl.multiple_of(block * rows, rows), rows)
        return (pltpu.make_async_copy(ug_hbm.at[:, cols], ug.at[b], u_sem.at[b, 0]),
                pltpu.make_async_copy(uu_hbm.at[:, cols], uu.at[b], u_sem.at[b, 1]))

    def store_u(s, b):
        cols = pl.ds(pl.multiple_of(s * rows, rows), rows)
        return (pltpu.make_async_copy(dug.at[b], dug_all.at[:, cols], o_sem.at[b, 0]),
                pltpu.make_async_copy(duu.at[b], duu_all.at[:, cols], o_sem.at[b, 1]))

    def y_first(d, h):
        land = 2 * (LEFT, RIGHT)[d]
        return remote(gy_hbm.at[half_of(h)], gy.at[land, half_of(h)], ys.at[d, h], yr.at[land, h], (right, left)[d])

    def y_second(d):
        src, h = 2 * (LEFT, RIGHT)[d], d
        return remote(gy.at[src, half_of(h)], gy.at[2 * FAR, half_of(h)], ys.at[d, 2], yr.at[2 * FAR, h],
                      (right, left)[d])

    def y_swap(slot, h):
        src = gy_hbm.at[half_of(h)] if slot == OWN else gy.at[2 * slot, half_of(h)]
        return remote(src, gy.at[2 * slot + 1, half_of(h)], yd.at[slot, h], yr.at[2 * slot + 1, h], other)

    def y_own(h):
        return pltpu.make_async_copy(gy_hbm.at[half_of(h)], gy.at[0, half_of(h)], yr.at[0, h])

    def x_first(d, h):
        land = 2 * (LEFT, RIGHT)[d]
        return remote(x_hbm.at[half_of(h)], x_at(land, h), xs.at[d, h], xr.at[land, h],
                      (right, left)[d])

    def x_second(d):
        src, h = 2 * (LEFT, RIGHT)[d], d
        return remote(x_at(src, h), x_at(2 * FAR, h), xs.at[d, 2], xr.at[2 * FAR, h], (right, left)[d])

    def x_swap(slot, h):
        src = x_hbm.at[half_of(h)] if slot == OWN else x_at(2 * slot, h)
        return remote(src, x_at(2 * slot + 1, h), xd.at[slot, h], xr.at[2 * slot + 1, h], other)

    x_in_copy = pltpu.make_async_copy(x_hbm, buf.at[part + FAR], b_sem.at[0])
    x_out_copy = pltpu.make_async_copy(buf.at[part + FAR], x_all.at[pl.ds(0, rows)], b_sem.at[1])

    def p_swap(slot):
        return remote(buf.at[2 * slot + 1], prec.at[slot], ps.at[slot], pr.at[slot], other)

    def r_first(d):
        return remote(buf.at[part + FAR, half_of(d)], hop.at[d], hs.at[d], hr.at[d], (right, left)[d])

    def r_last(d, h):
        src = part + (RIGHT, LEFT)[d]
        return remote(buf.at[src, half_of(h)], fin.at[d, half_of(h)], fs.at[d, h], fr.at[d, h], (right, left)[d])

    def r_final(d, q):
        rws = pl.ds(d * half + q * quarter, quarter)
        return remote(buf.at[part + (RIGHT, LEFT)[d], rws], fin.at[d, rws], qs.at[d, q], qr.at[d, q],
                      (right, left)[d])

    def s_swap(h, q):
        return remote(buf.at[2, pl.ds(h * half + q * quarter, quarter)],
                      (other_top, other_low)[h].at[pl.ds(q * quarter, quarter)], ss.at[h, q], sr.at[h, q], other)

    def s_first(d, q):
        return remote(buf.at[2, pl.ds(d * half + q * quarter, quarter)],
                      (left_top, right_low)[d].at[pl.ds(q * quarter, quarter)], as_.at[d, q], ar.at[d, q],
                      (right, left)[d])

    def s_out(h, q):
        return pltpu.make_async_copy(buf.at[2, pl.ds(h * half + q * quarter, quarter)],
                                     ((ds_top_a, ds_top_b), (ds_low_a, ds_low_b))[h][q // 2].at[
                                         pl.ds(q % 2 * quarter, quarter)], ds_sem.at[h, q])

    weights = [pltpu.make_async_copy(a, b, w_sem.at[i])
               for i, (a, b) in enumerate(((wd_hbm, wd), (wg_hbm, wg), (wu_hbm, wu)))]
    gw_copies = [pltpu.make_async_copy(acc, a, w_sem.at[i]) for i, a in enumerate((gwd_hbm, gwg_hbm, gwu_hbm))]

    barrier = pltpu.get_barrier_semaphore()
    for peer in (right, left, other):
        pl.semaphore_signal(barrier, inc=1, device_id={"tp": peer}, device_id_type=MESH)
    for h in (0, 1):
        y_own(h).start()
    weights[0].start()
    for c in load_u(0, 0):
        c.start()
    weights[1].start()
    weights[2].start()
    x_in_copy.start()
    pl.semaphore_wait(barrier, 3)
    for step in (0, 1):
        y_first(0, step).start()
        y_first(1, 1 - step).start()
    for h in (0, 1):
        y_swap(OWN, h).start()

    fstep = ffn // 5

    def clear():
        def body(i, carry):
            acc[pl.ds(pl.multiple_of(i * 16, 16), 16), :] = jnp.zeros((16, acc.shape[1]), F32)
            return carry

        lax.fori_loop(0, ffn // 16, body, 0)

    def accumulate(a, b):
        for f in range(5):
            lines = pl.ds(f * fstep, fstep)
            acc[lines, :] += jnp.dot(a[lines, :], b[...], preferred_element_type=F32)

    clear()
    for c in weights:
        c.wait()

    def unit(s, carry):
        slot, plane, b = s // 2, lax.rem(s, 2), lax.rem(s, 2)

        @pl.when(s + 1 < 8)
        def _():
            for c in load_u(s + 1, lax.rem(s + 1, 2)):
                c.start()

        @pl.when(s == 2)
        def _():
            y_first(0, 0).wait_recv()
            y_second(0).start()
            y_first(1, 1).wait_recv()
            y_second(1).start()
            y_swap(LEFT, 0).start()
            y_swap(RIGHT, 1).start()
            for step in (0, 1):
                x_first(0, step).start()
                x_first(1, 1 - step).start()
            x_in_copy.wait()
            x_out_copy.start()
            for k in (0, 1):
                x_swap(OWN, k).start()
            y_first(1, 0).wait_recv()
            y_swap(RIGHT, 0).start()
            y_first(0, 1).wait_recv()
            y_swap(LEFT, 1).start()

        @pl.when(s == 6)
        def _():
            x_out_copy.wait()
            for k in (0, 1):
                y_second(k).wait_recv()
                y_swap(FAR, k).start()

        @pl.when(s == 7)
        def _():
            for d in (0, 1):
                x_first(d, d).wait_recv()
                x_second(d).start()
                x_swap((LEFT, RIGHT)[d], d).start()

        @pl.when(jnp.logical_or(s == 0, plane == 1))
        def _():
            for h in (0, 1):
                pltpu.make_async_copy(gy_hbm.at[half_of(h)], gy.at[s, half_of(h)], yr.at[s, h]).wait()

        for c in load_u(s, b):
            c.wait()

        @pl.when(s >= 2)
        def _():
            for c in store_u(s - 2, b):
                c.wait()

        for f in range(2):
            lines = pl.ds(f * (ffn // 2), ffn // 2)
            grad_h = dot_cols(wd[lines, :], gy[s])
            gate_f = ug[b, lines, :].astype(F32)
            up_f = uu[b, lines, :].astype(F32)
            sig_gate = jax.nn.sigmoid(gate_f)
            act_gate = gate_f * sig_gate
            silu_grad = sig_gate * (1.0 + gate_f * (1.0 - sig_gate))
            z[lines, :] = (act_gate * up_f).astype(BF16)
            duu[b, lines, :] = (grad_h * act_gate).astype(BF16)
            dug[b, lines, :] = (grad_h * up_f * silu_grad).astype(BF16)

        for c in store_u(s, b):
            c.start()
        accumulate(z, gy.at[s])
        to = plane * s + (1 - plane) * (part + slot)
        for h in (0, 1):
            buf[to, half_of(h), :] = (dot_rows(dug[b, :, half_of(h)], wg[...])
                                      + dot_rows(duu[b, :, half_of(h)], wu[...])).astype(BF16)

        @pl.when(plane == 1)
        def _():
            remote(buf.at[s], prec.at[slot], ps.at[slot], pr.at[slot], other).start()

        return carry

    lax.fori_loop(0, 8, unit, 0)
    gw_copies[0].start()

    def add_into(slot, row, src, at, count):
        step = 64

        def body(i, carry):
            to = pl.ds(pl.multiple_of(row + i * step, step), step)
            frm = pl.ds(pl.multiple_of(at + i * step, step), step)
            buf[slot, to, :] = (buf[slot, to, :].astype(F32) + src[frm, :].astype(F32)).astype(BF16)
            return carry

        lax.fori_loop(0, count // step, body, 0)

    p_swap(FAR).wait_recv()
    for d in (0, 1):
        add_into(part + FAR, d * half, prec.at[FAR], d * half, half)
        r_first(d).start()
    for d, slot in ((0, RIGHT), (1, LEFT)):
        p_swap(slot).wait_recv()
        add_into(part + slot, (1 - d) * half, prec.at[slot], (1 - d) * half, half)
        r_last(d, 1 - d).start()
    for d, slot in ((0, RIGHT), (1, LEFT)):
        add_into(part + slot, d * half, prec.at[slot], d * half, half)
    p_swap(OWN).wait_recv()
    add_into(part + OWN, 0, prec.at[OWN], 0, rows)
    for s in (6, 7):
        for c in store_u(s, s % 2):
            c.wait()
    for d in (0, 1):
        x_first(d, 1 - d).wait_recv()
        x_swap((LEFT, RIGHT)[d], 1 - d).start()
    p_swap(OWN).wait_send()
    p_swap(RIGHT).wait_send()
    for h in (0, 1):
        for slot in range(3):
            x_swap(slot, h).wait_recv()

    def x_load(s, b):
        return pltpu.make_async_copy(x_all.at[pl.ds(pl.multiple_of(s * rows, rows), rows)], buf.at[1 + 2 * b],
                                     u_sem.at[b, 0])

    def d_load(src, s, b):
        return pltpu.make_async_copy(src.at[:, pl.ds(pl.multiple_of(s * rows, rows), rows)], dug.at[b],
                                     u_sem.at[b, 1])

    def start_loads(t):
        b = lax.rem(t, 2)
        x_load(lax.rem(t, 8), b).start()

        @pl.when(t < 8)
        def _():
            d_load(dug_all, t, b).start()

        @pl.when(t >= 8)
        def _():
            d_load(duu_all, t - 8, b).start()

    start_loads(0)
    gw_copies[0].wait()
    clear()

    def step_w(t, carry):
        b = lax.rem(t, 2)

        @pl.when(t == 5)
        def _():
            for d in (0, 1):
                x_second(d).wait_recv()
                x_swap(FAR, d).start()

        @pl.when(t == 6)
        def _():
            for h in (0, 1):
                x_swap(FAR, h).wait_recv()

        @pl.when(t + 1 < 16)
        def _():
            start_loads(t + 1)

        @pl.when(t == 8)
        def _():
            gw_copies[1].start()
            gw_copies[1].wait()
            clear()

        x_load(lax.rem(t, 8), b).wait()
        d_load(dug_all, lax.rem(t, 8), b).wait()
        accumulate(dug.at[b], buf.at[1 + 2 * b])
        return carry

    lax.fori_loop(0, 16, step_w, 0)
    gw_copies[2].start()

    norm_loads = (pltpu.make_async_copy(xin_hbm, buf.at[0], b_sem.at[0]),
                  pltpu.make_async_copy(gres_hbm, buf.at[1], b_sem.at[1]))
    for c in norm_loads:
        c.start()
    for h in (0, 1):
        y_swap(RIGHT, h).wait_send()
    y_second(1).wait_send()
    for d in (0, 1):
        r_first(d).wait_recv()
    for q in range(4):
        for d, slot in ((0, RIGHT), (1, LEFT)):
            add_into(part + slot, d * half + q * quarter, hop.at[d], q * quarter, quarter)
            r_final(d, q).start()
    for c in norm_loads:
        c.wait()
    for d in (0, 1):
        r_last(d, 1 - d).wait_recv()
    step = 32
    gamma_f = gamma_ref[...].astype(F32).reshape(1, buf.shape[2])

    def norm_rows(row):
        def norm(i, carry):
            r = pl.ds(pl.multiple_of(row + i * step, step), step)
            grad_x = (buf[part, r, :].astype(F32) + fin[0, r, :].astype(F32) + fin[1, r, :].astype(F32)).astype(BF16)
            xin_f = buf[0, r, :].astype(F32)
            inv_rms = lax.rsqrt(jnp.mean(xin_f * xin_f, axis=-1, keepdims=True) + NORM_EPS)
            scaled = grad_x.astype(F32) * gamma_f
            proj_mean = jnp.mean(scaled * xin_f, axis=-1, keepdims=True)
            buf[2, r, :] = (buf[1, r, :].astype(F32)
                            + inv_rms * (scaled - xin_f * (inv_rms * inv_rms) * proj_mean)).astype(BF16)
            return carry

        lax.fori_loop(0, quarter // step, norm, 0)

    for q in range(4):
        for h in (0, 1):
            r_final(h, q).wait_recv()
            norm_rows(h * half + q * quarter)
            s_out(h, q).start()
            s_first(h, q).start()
            s_swap(h, q).start()

    for d in (0, 1):
        for h in (0, 1):
            y_first(d, h).wait_send()
            x_first(d, h).wait_send()
        r_last(d, 1 - d).wait_send()
        x_second(d).wait_send()
        r_first(d).wait_send()
    y_second(0).wait_send()
    for h in (0, 1):
        for slot in range(4):
            if slot != RIGHT:
                y_swap(slot, h).wait_send()
            x_swap(slot, h).wait_send()
        for q in range(4):
            r_final(h, q).wait_send()
            s_swap(h, q).wait_send()
            s_swap(h, q).wait_recv()
            s_out(h, q).wait()
            s_first(h, q).wait_send()
            s_first(h, q).wait_recv()
    for slot in (LEFT, FAR):
        p_swap(slot).wait_send()
    gw_copies[2].wait()


def settle_kernel(*refs):
    held, load_sem, store_sem = refs[-3:]
    arrays = (len(refs) - 3) // 2
    slots, lines = held.shape[0], held.shape[1]
    pieces = [(a, i) for a in range(arrays) for i in range(refs[a].shape[0] // lines)]
    lag = slots // 2

    def load(k):
        a, i = pieces[k]
        return pltpu.make_async_copy(refs[a].at[pl.ds(i * lines, lines)], held.at[k % slots], load_sem.at[k % slots])

    def store(k):
        a, i = pieces[k]
        return pltpu.make_async_copy(held.at[k % slots], refs[arrays + a].at[pl.ds(i * lines, lines)],
                                     store_sem.at[k % slots])

    for k in range(slots):
        load(k).start()
    for k in range(len(pieces)):
        if k >= lag:
            store(k - lag).wait()
            if k - lag + slots < len(pieces):
                load(k - lag + slots).start()
        load(k).wait()
        store(k).start()
    for k in range(len(pieces) - lag, len(pieces)):
        store(k).wait()


def attn_kernel(n, pieces, rows, *refs):
    count = len(pieces)
    parts = refs[:count]
    held, ot, wo, do, gwo, h_sem, l_sem, o_sem = refs[-8:]
    rest = refs[count:-8]
    ot_hbm, wo_hbm = rest[:2]
    do_hbm, gwo_hbm = rest[-2:]
    begins = pieces[0][0] == OWN
    me = lax.axis_index("tp")
    core, chip, chips = lax.rem(me, 2), me // 2, n // 2
    ends = [sum(p.shape[0] for p in parts[:i + 1]) for i in range(count)]

    def here(i):
        return pl.ds(ends[i] - parts[i].shape[0], parts[i].shape[0])

    def there(i):
        slot, plane, row = pieces[i]
        block = lax.rem(chip + chip_step(slot), chips) * 2 + lax.rem(core + plane, 2)
        return pl.ds(pl.multiple_of(block * rows + row, 128), parts[i].shape[0])

    loads = [(pltpu.make_async_copy(parts[i], held.at[here(i)], h_sem.at[i]),
              pltpu.make_async_copy(ot_hbm.at[:, there(i)], ot.at[:, here(i)], l_sem.at[2 + i])) for i in range(count)]
    wo_load = pltpu.make_async_copy(wo_hbm, wo, l_sem.at[0])
    gwo_load = None if begins else pltpu.make_async_copy(rest[2], gwo, l_sem.at[1])
    wo_load.start()
    for i in range(count):
        for c in loads[i]:
            c.start()
        if ends[i] == rows and gwo_load is not None:
            gwo_load.start()
    wo_load.wait()
    outs = []
    done = 0
    for low in range(0, ends[-1], rows):
        first = done
        while done < count and ends[done] <= low + rows:
            for c in loads[done]:
                c.wait()
            done += 1
        now = pl.ds(low, rows)
        if begins and low == 0:
            outs.append(pltpu.make_async_copy(held.at[now], rest[2], o_sem.at[count + 1]))
            outs[-1].start()
        do[:, now] = dot_cols(wo[...], held[now, :]).astype(BF16)
        for i in range(first, done):
            outs.append(pltpu.make_async_copy(do.at[:, here(i)], do_hbm.at[:, there(i)], o_sem.at[i]))
            outs[-1].start()
        if low == 0 and gwo_load is not None:
            gwo_load.wait()
        share = jnp.dot(ot[:, now], held[now, :], preferred_element_type=F32)
        gwo[...] = share if begins and low == 0 else gwo[...] + share
    outs.append(pltpu.make_async_copy(gwo, gwo_hbm, o_sem.at[count]))
    outs[-1].start()
    for c in outs:
        c.wait()


def solution(mesh):
    n = mesh.shape["tp"]
    chips = n // 2
    right_of = [(i, ((i // 2 + 1) % chips) * 2 + i % 2) for i in range(n)]
    partner_of = [(i, i ^ 1) for i in range(n)]
    left_of = [(i, ((i // 2 - 1) % chips) * 2 + i % 2) for i in range(n)]

    def go_right(a):
        return lax.ppermute(a, "tp", right_of)

    def go_left(a):
        return lax.ppermute(a, "tp", left_of)

    def swap(a):
        return lax.ppermute(a, "tp", partner_of)

    token_spec = P(("dp", "tp"), None)
    split_cols = P("dp", "tp")
    weight_cols = P(None, "tp")
    weight_rows = P("tp", None)

    def run_main(x_norm, grad_y, u_gate_t, u_up_t, w_gate_t, w_up_t, w_down, x_in, gamma, grad_res):
        rows, hidden = x_norm.shape
        ffn, tokens = u_gate_t.shape
        half = rows // 2
        any_spec = pl.BlockSpec(memory_space=pl.ANY)
        dma = pltpu.SemaphoreType.DMA
        return pl.pallas_call(
            functools.partial(main_kernel, n),
            out_shape=[jax.ShapeDtypeStruct(*a) for a in (
                ((tokens, hidden), BF16), ((ffn, tokens), BF16), ((ffn, tokens), BF16),
                ((ffn, hidden), F32), ((ffn, hidden), F32), ((ffn, hidden), F32),
                *[((half // 2, hidden), BF16)] * 4, *[((half, hidden), BF16)] * 4)],
            in_specs=[any_spec] * 8 + [pl.BlockSpec(memory_space=pltpu.VMEM), any_spec],
            out_specs=[any_spec] * 14,
            scratch_shapes=[
                pltpu.VMEM((ffn, hidden), BF16), pltpu.VMEM((ffn, hidden), BF16), pltpu.VMEM((ffn, hidden), BF16),
                pltpu.VMEM((12, rows, hidden), BF16),
                pltpu.VMEM((2, ffn, rows), BF16), pltpu.VMEM((2, ffn, rows), BF16),
                pltpu.VMEM((ffn, rows), BF16), pltpu.VMEM((2, ffn, rows), BF16), pltpu.VMEM((2, ffn, rows), BF16),
                pltpu.VMEM((ffn, hidden), F32), pltpu.VMEM((4, rows, hidden), BF16),
                pltpu.VMEM((2, half, hidden), BF16), pltpu.VMEM((2, rows, hidden), BF16),
                dma((3,)), dma((2, 2)), dma((2, 4)), dma((2,)),
                dma((2, 3)), dma((4, 2)), dma((8, 2)),
                dma((2, 3)), dma((4, 2)), dma((8, 2)),
                dma((4,)), dma((4,)), dma((2,)), dma((2,)), dma((2, 2)), dma((2, 2)),
                dma((2, 4)), dma((2, 4)), dma((2, 4)), dma((2, 4)), dma((2, 4)),
                dma((2, 4)), dma((2, 4)),
            ],
            compiler_params=pltpu.CompilerParams(collective_id=0, has_side_effects=True,
                                                 vmem_limit_bytes=67_000_000),
        )(x_norm, grad_y, u_gate_t, u_up_t, w_gate_t, w_up_t, w_down, x_in, gamma, grad_res)

    any_space = pl.BlockSpec(memory_space=pl.ANY)

    def settle(*arrays):
        lines, hidden = arrays[0].shape
        slots = min(16, 10 * len(arrays))
        return pl.pallas_call(
            settle_kernel,
            in_specs=[any_space] * len(arrays), out_specs=[any_space] * len(arrays),
            out_shape=[jax.ShapeDtypeStruct(a.shape, a.dtype) for a in arrays],
            scratch_shapes=[pltpu.VMEM((slots, lines // 10, hidden), F32), pltpu.SemaphoreType.DMA((slots,)),
                            pltpu.SemaphoreType.DMA((slots,))],
            cost_estimate=pl.CostEstimate(flops=2000 * len(arrays) * lines * hidden,
                                          bytes_accessed=8 * len(arrays) * lines * hidden, transcendentals=0),
            compiler_params=pltpu.CompilerParams(vmem_limit_bytes=67_000_000),
        )(*arrays)

    def attn(pieces, rows, attn_t, w_out, *sofar):
        arrays, kinds = [p[0] for p in pieces], tuple(p[1:] for p in pieces)
        hidden, (width, tokens) = arrays[0].shape[1], attn_t.shape
        total, count = sum(a.shape[0] for a in arrays), len(arrays)
        dma = pltpu.SemaphoreType.DMA
        results = [jax.ShapeDtypeStruct((width, tokens), BF16), jax.ShapeDtypeStruct((width, hidden), F32)]
        if not sofar:
            results.insert(0, jax.ShapeDtypeStruct((rows, hidden), BF16))
        return pl.pallas_call(
            functools.partial(attn_kernel, n, kinds, rows),
            in_specs=[any_space] * (count + 2 + len(sofar)), out_specs=[any_space] * len(results),
            scratch_shapes=[
                pltpu.VMEM((total, hidden), BF16), pltpu.VMEM((width, total), BF16), pltpu.VMEM((width, hidden), BF16),
                pltpu.VMEM((width, total), BF16), pltpu.VMEM((width, hidden), F32),
                dma((count,)), dma((2 + count,)), dma((2 + count,))],
            out_shape=results,
            input_output_aliases={count + 3: 0} if sofar else {},
            cost_estimate=pl.CostEstimate(flops=1200 * total * hidden, bytes_accessed=8 * total * hidden,
                                          transcendentals=0),
            compiler_params=pltpu.CompilerParams(vmem_limit_bytes=67_000_000),
        )(*arrays, attn_t, w_out, *sofar)

    def local_backward(x_norm, grad_y, u_gate, u_up, w_gate, w_up, w_down, x_in, gamma, grad_res, attn_out, w_out):
        attn_t = attn_out.T
        rows = x_norm.shape[0]
        half, part = rows // 2, rows // 4
        (_, _, _, gate_t, up_t, down, top_a, top_b, low_a, low_b, other_top, other_low, left_top,
         right_low) = run_main(
            x_norm, grad_y, u_gate.T, u_up.T, w_gate.T, w_up.T, w_down, x_in, gamma, grad_res)

        def both(a, other, slot, row):
            return [(a, slot, 0, row), (other, slot, 1, row)]

        far_top, far_low = go_right(left_top), go_left(right_low)
        left_low_a, right_top_a = go_right(low_a), go_left(top_a)
        left_low_b, right_top_b = go_right(low_b), go_left(top_b)
        left_top_other, right_low_other = swap(left_top), swap(right_low)
        gate_t, up_t = settle(gate_t, up_t)
        grad_sum, do_t, gwo = attn([
            (top_a, OWN, 0, 0), (top_b, OWN, 0, part), (low_a, OWN, 0, half), (low_b, OWN, 0, half + part),
            (other_top, OWN, 1, 0), (other_low, OWN, 1, half),
            *both(left_top, left_top_other, LEFT, 0), *both(right_low, right_low_other, RIGHT, half)],
            rows, attn_t, w_out)
        gw_down, = settle(down)
        far_top_other, far_low_other = swap(far_top), swap(far_low)
        left_low_a_other, right_top_a_other = swap(left_low_a), swap(right_top_a)
        do_t, gwo = attn([
            *both(far_top, far_top_other, FAR, 0), *both(far_low, far_low_other, FAR, half),
            *both(left_low_a, left_low_a_other, LEFT, half), *both(right_top_a, right_top_a_other, RIGHT, 0)],
            rows, attn_t, w_out, gwo, do_t)
        left_low_b_other, right_top_b_other = swap(left_low_b), swap(right_top_b)
        do_t, gwo = attn([
            *both(left_low_b, left_low_b_other, LEFT, half + part),
            *both(right_top_b, right_top_b_other, RIGHT, part)], rows, attn_t, w_out, gwo, do_t)
        return grad_sum, do_t.T, gate_t.T, up_t.T, gw_down, gwo

    return jax.shard_map(
        local_backward,
        mesh=mesh,
        in_specs=(token_spec, token_spec, split_cols, split_cols, weight_cols, weight_cols, weight_rows,
                  token_spec, P(None), token_spec, split_cols, weight_rows),
        out_specs=(token_spec, split_cols, split_cols, split_cols, token_spec, token_spec),
        check_vma=False,
    )
```

```python
import functools

import jax
import jax.numpy as jnp
from jax import lax
from jax.experimental import pallas as pl
from jax.experimental.pallas import tpu as pltpu
from jax.sharding import PartitionSpec as P


NORM_EPS = 1e-5
CONTRACT_ROWS = (((0,), (0,)), ((), ()))
CONTRACT_COLS = (((1,), (1,)), ((), ()))
F32, BF16 = jnp.float32, jnp.bfloat16
MESH = pl.DeviceIdType.MESH
OWN, RIGHT, LEFT, FAR = range(4)


def dot_rows(a, b):
    return lax.dot_general(a, b, CONTRACT_ROWS, preferred_element_type=F32)


def dot_cols(a, b):
    return lax.dot_general(a, b, CONTRACT_COLS, preferred_element_type=F32)


def chip_step(slot):
    return lax.rem(slot * (slot + 1) // 2, 4)


def main_kernel(n, x_hbm, gy_hbm, ug_hbm, uu_hbm, wg_hbm, wu_hbm, wd_hbm, xin_hbm, gamma_ref, gres_hbm,
                x_all, dug_all, duu_all, gwg_hbm, gwu_hbm, gwd_hbm, ds_top_a, ds_top_b, ds_low_a, ds_low_b,
                other_top, other_low, left_top, right_low,
                wg, wu, wd, buf, ug, uu, z, dug, duu, acc, prec, hop, fin,
                w_sem, u_sem, o_sem, b_sem, ys, yd, yr, xs, xd, xr, ps, pr, hs, hr, fs, fr, qs, qr, ss, sr, ds_sem,
                as_, ar):
    me = lax.axis_index("tp")
    core, chip, chips = lax.rem(me, 2), me // 2, n // 2
    right = lax.rem(chip + 1, chips) * 2 + core
    left = lax.rem(chip + chips - 1, chips) * 2 + core
    other = chip * 2 + 1 - core
    rows = gy_hbm.shape[0]
    half = rows // 2
    quarter = half // 4
    ffn = wd.shape[0]
    gy = buf
    part = 8

    def half_of(h):
        return pl.ds(h * half, half)

    def x_at(slot, h):
        return x_all.at[pl.ds(slot * rows + h * half, half)]

    def remote(src, dst, send, recv, to):
        return pltpu.make_async_remote_copy(src_ref=src, dst_ref=dst, send_sem=send, recv_sem=recv,
                                            device_id={"tp": to}, device_id_type=MESH)

    def load_u(s, b):
        block = lax.rem(chip + chip_step(s // 2), chips) * 2 + lax.rem(core + lax.rem(s, 2), 2)
        cols = pl.ds(pl.multiple_of(block * rows, rows), rows)
        return (pltpu.make_async_copy(ug_hbm.at[:, cols], ug.at[b], u_sem.at[b, 0]),
                pltpu.make_async_copy(uu_hbm.at[:, cols], uu.at[b], u_sem.at[b, 1]))

    def store_u(s, b):
        cols = pl.ds(pl.multiple_of(s * rows, rows), rows)
        return (pltpu.make_async_copy(dug.at[b], dug_all.at[:, cols], o_sem.at[b, 0]),
                pltpu.make_async_copy(duu.at[b], duu_all.at[:, cols], o_sem.at[b, 1]))

    def y_first(d, h):
        land = 2 * (LEFT, RIGHT)[d]
        return remote(gy_hbm.at[half_of(h)], gy.at[land, half_of(h)], ys.at[d, h], yr.at[land, h], (right, left)[d])

    def y_second(d):
        src, h = 2 * (LEFT, RIGHT)[d], d
        return remote(gy.at[src, half_of(h)], gy.at[2 * FAR, half_of(h)], ys.at[d, 2], yr.at[2 * FAR, h],
                      (right, left)[d])

    def y_swap(slot, h):
        src = gy_hbm.at[half_of(h)] if slot == OWN else gy.at[2 * slot, half_of(h)]
        return remote(src, gy.at[2 * slot + 1, half_of(h)], yd.at[slot, h], yr.at[2 * slot + 1, h], other)

    def y_own(h):
        return pltpu.make_async_copy(gy_hbm.at[half_of(h)], gy.at[0, half_of(h)], yr.at[0, h])

    def x_first(d, h):
        land = 2 * (LEFT, RIGHT)[d]
        return remote(x_hbm.at[half_of(h)], x_at(land, h), xs.at[d, h], xr.at[land, h],
                      (right, left)[d])

    def x_second(d):
        src, h = 2 * (LEFT, RIGHT)[d], d
        return remote(x_at(src, h), x_at(2 * FAR, h), xs.at[d, 2], xr.at[2 * FAR, h], (right, left)[d])

    def x_swap(slot, h):
        src = x_hbm.at[half_of(h)] if slot == OWN else x_at(2 * slot, h)
        return remote(src, x_at(2 * slot + 1, h), xd.at[slot, h], xr.at[2 * slot + 1, h], other)

    x_in_copy = pltpu.make_async_copy(x_hbm, buf.at[part + FAR], b_sem.at[0])
    x_out_copy = pltpu.make_async_copy(buf.at[part + FAR], x_all.at[pl.ds(0, rows)], b_sem.at[1])

    def p_swap(slot):
        return remote(buf.at[2 * slot + 1], prec.at[slot], ps.at[slot], pr.at[slot], other)

    def r_first(d):
        return remote(buf.at[part + FAR, half_of(d)], hop.at[d], hs.at[d], hr.at[d], (right, left)[d])

    def r_last(d, h):
        src = part + (RIGHT, LEFT)[d]
        return remote(buf.at[src, half_of(h)], fin.at[d, half_of(h)], fs.at[d, h], fr.at[d, h], (right, left)[d])

    def r_final(d, q):
        rws = pl.ds(d * half + q * quarter, quarter)
        return remote(buf.at[part + (RIGHT, LEFT)[d], rws], fin.at[d, rws], qs.at[d, q], qr.at[d, q],
                      (right, left)[d])

    def s_swap(h, q):
        return remote(buf.at[2, pl.ds(h * half + q * quarter, quarter)],
                      (other_top, other_low)[h].at[pl.ds(q * quarter, quarter)], ss.at[h, q], sr.at[h, q], other)

    def s_first(d, q):
        return remote(buf.at[2, pl.ds(d * half + q * quarter, quarter)],
                      (left_top, right_low)[d].at[pl.ds(q * quarter, quarter)], as_.at[d, q], ar.at[d, q],
                      (right, left)[d])

    def s_out(h, q):
        return pltpu.make_async_copy(buf.at[2, pl.ds(h * half + q * quarter, quarter)],
                                     ((ds_top_a, ds_top_b), (ds_low_a, ds_low_b))[h][q // 2].at[
                                         pl.ds(q % 2 * quarter, quarter)], ds_sem.at[h, q])

    weights = [pltpu.make_async_copy(a, b, w_sem.at[i])
               for i, (a, b) in enumerate(((wd_hbm, wd), (wg_hbm, wg), (wu_hbm, wu)))]
    gw_copies = [pltpu.make_async_copy(acc, a, w_sem.at[i]) for i, a in enumerate((gwd_hbm, gwg_hbm, gwu_hbm))]

    barrier = pltpu.get_barrier_semaphore()
    for peer in (right, left, other):
        pl.semaphore_signal(barrier, inc=1, device_id={"tp": peer}, device_id_type=MESH)
    for h in (0, 1):
        y_own(h).start()
    weights[0].start()
    for c in load_u(0, 0):
        c.start()
    weights[1].start()
    weights[2].start()
    x_in_copy.start()
    pl.semaphore_wait(barrier, 3)
    for step in (0, 1):
        y_first(0, step).start()
        y_first(1, 1 - step).start()
    for h in (0, 1):
        y_swap(OWN, h).start()

    fstep = ffn // 5

    def clear():
        def body(i, carry):
            acc[pl.ds(pl.multiple_of(i * 16, 16), 16), :] = jnp.zeros((16, acc.shape[1]), F32)
            return carry

        lax.fori_loop(0, ffn // 16, body, 0)

    def accumulate(a, b):
        for f in range(5):
            lines = pl.ds(f * fstep, fstep)
            acc[lines, :] += jnp.dot(a[lines, :], b[...], preferred_element_type=F32)

    clear()
    for c in weights:
        c.wait()

    def unit(s, carry):
        slot, plane, b = s // 2, lax.rem(s, 2), lax.rem(s, 2)

        @pl.when(s + 1 < 8)
        def _():
            for c in load_u(s + 1, lax.rem(s + 1, 2)):
                c.start()

        @pl.when(s == 2)
        def _():
            y_first(0, 0).wait_recv()
            y_second(0).start()
            y_first(1, 1).wait_recv()
            y_second(1).start()
            y_swap(LEFT, 0).start()
            y_swap(RIGHT, 1).start()
            for step in (0, 1):
                x_first(0, step).start()
                x_first(1, 1 - step).start()
            x_in_copy.wait()
            x_out_copy.start()
            for k in (0, 1):
                x_swap(OWN, k).start()
            y_first(1, 0).wait_recv()
            y_swap(RIGHT, 0).start()
            y_first(0, 1).wait_recv()
            y_swap(LEFT, 1).start()

        @pl.when(s == 6)
        def _():
            x_out_copy.wait()
            for k in (0, 1):
                y_second(k).wait_recv()
                y_swap(FAR, k).start()

        @pl.when(s == 7)
        def _():
            for d in (0, 1):
                x_first(d, d).wait_recv()
                x_second(d).start()
                x_swap((LEFT, RIGHT)[d], d).start()

        @pl.when(jnp.logical_or(s == 0, plane == 1))
        def _():
            for h in (0, 1):
                pltpu.make_async_copy(gy_hbm.at[half_of(h)], gy.at[s, half_of(h)], yr.at[s, h]).wait()

        for c in load_u(s, b):
            c.wait()

        @pl.when(s >= 2)
        def _():
            for c in store_u(s - 2, b):
                c.wait()

        for f in range(2):
            lines = pl.ds(f * (ffn // 2), ffn // 2)
            grad_h = dot_cols(wd[lines, :], gy[s])
            gate_f = ug[b, lines, :].astype(F32)
            up_f = uu[b, lines, :].astype(F32)
            sig_gate = jax.nn.sigmoid(gate_f)
            act_gate = gate_f * sig_gate
            silu_grad = sig_gate * (1.0 + gate_f * (1.0 - sig_gate))
            z[lines, :] = (act_gate * up_f).astype(BF16)
            duu[b, lines, :] = (grad_h * act_gate).astype(BF16)
            dug[b, lines, :] = (grad_h * up_f * silu_grad).astype(BF16)

        for c in store_u(s, b):
            c.start()
        accumulate(z, gy.at[s])
        to = plane * s + (1 - plane) * (part + slot)
        for h in (0, 1):
            buf[to, half_of(h), :] = (dot_rows(dug[b, :, half_of(h)], wg[...])
                                      + dot_rows(duu[b, :, half_of(h)], wu[...])).astype(BF16)

        @pl.when(plane == 1)
        def _():
            remote(buf.at[s], prec.at[slot], ps.at[slot], pr.at[slot], other).start()

        return carry

    lax.fori_loop(0, 8, unit, 0)
    gw_copies[0].start()

    def add_into(slot, row, src, at, count):
        step = 64

        def body(i, carry):
            to = pl.ds(pl.multiple_of(row + i * step, step), step)
            frm = pl.ds(pl.multiple_of(at + i * step, step), step)
            buf[slot, to, :] = (buf[slot, to, :].astype(F32) + src[frm, :].astype(F32)).astype(BF16)
            return carry

        lax.fori_loop(0, count // step, body, 0)

    p_swap(FAR).wait_recv()
    for d in (0, 1):
        add_into(part + FAR, d * half, prec.at[FAR], d * half, half)
        r_first(d).start()
    for d, slot in ((0, RIGHT), (1, LEFT)):
        p_swap(slot).wait_recv()
        add_into(part + slot, (1 - d) * half, prec.at[slot], (1 - d) * half, half)
        r_last(d, 1 - d).start()
    for d, slot in ((0, RIGHT), (1, LEFT)):
        add_into(part + slot, d * half, prec.at[slot], d * half, half)
    p_swap(OWN).wait_recv()
    add_into(part + OWN, 0, prec.at[OWN], 0, rows)
    for s in (6, 7):
        for c in store_u(s, s % 2):
            c.wait()
    for d in (0, 1):
        x_first(d, 1 - d).wait_recv()
        x_swap((LEFT, RIGHT)[d], 1 - d).start()
    p_swap(OWN).wait_send()
    p_swap(RIGHT).wait_send()
    for h in (0, 1):
        for slot in range(3):
            x_swap(slot, h).wait_recv()

    def x_load(s, b):
        return pltpu.make_async_copy(x_all.at[pl.ds(pl.multiple_of(s * rows, rows), rows)], buf.at[1 + 2 * b],
                                     u_sem.at[b, 0])

    def d_load(src, s, b):
        return pltpu.make_async_copy(src.at[:, pl.ds(pl.multiple_of(s * rows, rows), rows)], dug.at[b],
                                     u_sem.at[b, 1])

    def start_loads(t):
        b = lax.rem(t, 2)
        x_load(lax.rem(t, 8), b).start()

        @pl.when(t < 8)
        def _():
            d_load(dug_all, t, b).start()

        @pl.when(t >= 8)
        def _():
            d_load(duu_all, t - 8, b).start()

    start_loads(0)
    gw_copies[0].wait()
    clear()

    def step_w(t, carry):
        b = lax.rem(t, 2)

        @pl.when(t == 5)
        def _():
            for d in (0, 1):
                x_second(d).wait_recv()
                x_swap(FAR, d).start()

        @pl.when(t == 6)
        def _():
            for h in (0, 1):
                x_swap(FAR, h).wait_recv()

        @pl.when(t + 1 < 16)
        def _():
            start_loads(t + 1)

        @pl.when(t == 8)
        def _():
            gw_copies[1].start()
            gw_copies[1].wait()
            clear()

        x_load(lax.rem(t, 8), b).wait()
        d_load(dug_all, lax.rem(t, 8), b).wait()
        accumulate(dug.at[b], buf.at[1 + 2 * b])
        return carry

    lax.fori_loop(0, 16, step_w, 0)
    gw_copies[2].start()

    norm_loads = (pltpu.make_async_copy(xin_hbm, buf.at[0], b_sem.at[0]),
                  pltpu.make_async_copy(gres_hbm, buf.at[1], b_sem.at[1]))
    for c in norm_loads:
        c.start()
    for h in (0, 1):
        y_swap(RIGHT, h).wait_send()
    y_second(1).wait_send()
    for d in (0, 1):
        r_first(d).wait_recv()
    for q in range(4):
        for d, slot in ((0, RIGHT), (1, LEFT)):
            add_into(part + slot, d * half + q * quarter, hop.at[d], q * quarter, quarter)
            r_final(d, q).start()
    for c in norm_loads:
        c.wait()
    for d in (0, 1):
        r_last(d, 1 - d).wait_recv()
    step = 32
    gamma_f = gamma_ref[...].astype(F32).reshape(1, buf.shape[2])

    def norm_rows(row):
        def norm(i, carry):
            r = pl.ds(pl.multiple_of(row + i * step, step), step)
            grad_x = (buf[part, r, :].astype(F32) + fin[0, r, :].astype(F32) + fin[1, r, :].astype(F32)).astype(BF16)
            xin_f = buf[0, r, :].astype(F32)
            inv_rms = lax.rsqrt(jnp.mean(xin_f * xin_f, axis=-1, keepdims=True) + NORM_EPS)
            scaled = grad_x.astype(F32) * gamma_f
            proj_mean = jnp.mean(scaled * xin_f, axis=-1, keepdims=True)
            buf[2, r, :] = (buf[1, r, :].astype(F32)
                            + inv_rms * (scaled - xin_f * (inv_rms * inv_rms) * proj_mean)).astype(BF16)
            return carry

        lax.fori_loop(0, quarter // step, norm, 0)

    for q in range(4):
        for h in (0, 1):
            r_final(h, q).wait_recv()
            norm_rows(h * half + q * quarter)
            s_out(h, q).start()
            s_first(h, q).start()
            s_swap(h, q).start()

    for d in (0, 1):
        for h in (0, 1):
            y_first(d, h).wait_send()
            x_first(d, h).wait_send()
        r_last(d, 1 - d).wait_send()
        x_second(d).wait_send()
        r_first(d).wait_send()
    y_second(0).wait_send()
    for h in (0, 1):
        for slot in range(4):
            if slot != RIGHT:
                y_swap(slot, h).wait_send()
            x_swap(slot, h).wait_send()
        for q in range(4):
            r_final(h, q).wait_send()
            s_swap(h, q).wait_send()
            s_swap(h, q).wait_recv()
            s_out(h, q).wait()
            s_first(h, q).wait_send()
            s_first(h, q).wait_recv()
    for slot in (LEFT, FAR):
        p_swap(slot).wait_send()
    gw_copies[2].wait()


def settle_kernel(*refs):
    held, load_sem, store_sem = refs[-3:]
    arrays = (len(refs) - 3) // 2
    slots, lines = held.shape[0], held.shape[1]
    pieces = [(a, i) for a in range(arrays) for i in range(refs[a].shape[0] // lines)]
    lag = slots // 2

    def load(k):
        a, i = pieces[k]
        return pltpu.make_async_copy(refs[a].at[pl.ds(i * lines, lines)], held.at[k % slots], load_sem.at[k % slots])

    def store(k):
        a, i = pieces[k]
        return pltpu.make_async_copy(held.at[k % slots], refs[arrays + a].at[pl.ds(i * lines, lines)],
                                     store_sem.at[k % slots])

    for k in range(slots):
        load(k).start()
    for k in range(len(pieces)):
        if k >= lag:
            store(k - lag).wait()
            if k - lag + slots < len(pieces):
                load(k - lag + slots).start()
        load(k).wait()
        store(k).start()
    for k in range(len(pieces) - lag, len(pieces)):
        store(k).wait()


def attn_kernel(n, pieces, rows, *refs):
    count = len(pieces)
    parts = refs[:count]
    held, ot, wo, do, gwo, h_sem, l_sem, o_sem = refs[-8:]
    rest = refs[count:-8]
    ot_hbm, wo_hbm = rest[:2]
    do_hbm, gwo_hbm = rest[-2:]
    begins = pieces[0][0] == OWN
    me = lax.axis_index("tp")
    core, chip, chips = lax.rem(me, 2), me // 2, n // 2
    ends = [sum(p.shape[0] for p in parts[:i + 1]) for i in range(count)]

    def here(i):
        return pl.ds(ends[i] - parts[i].shape[0], parts[i].shape[0])

    def there(i):
        slot, plane, row = pieces[i]
        block = lax.rem(chip + chip_step(slot), chips) * 2 + lax.rem(core + plane, 2)
        return pl.ds(pl.multiple_of(block * rows + row, 128), parts[i].shape[0])

    loads = [(pltpu.make_async_copy(parts[i], held.at[here(i)], h_sem.at[i]),
              pltpu.make_async_copy(ot_hbm.at[:, there(i)], ot.at[:, here(i)], l_sem.at[2 + i])) for i in range(count)]
    wo_load = pltpu.make_async_copy(wo_hbm, wo, l_sem.at[0])
    gwo_load = None if begins else pltpu.make_async_copy(rest[2], gwo, l_sem.at[1])
    wo_load.start()
    for i in range(count):
        for c in loads[i]:
            c.start()
        if ends[i] == rows and gwo_load is not None:
            gwo_load.start()
    wo_load.wait()
    outs = []
    done = 0
    for low in range(0, ends[-1], rows):
        first = done
        while done < count and ends[done] <= low + rows:
            for c in loads[done]:
                c.wait()
            done += 1
        now = pl.ds(low, rows)
        if begins and low == 0:
            outs.append(pltpu.make_async_copy(held.at[now], rest[2], o_sem.at[count + 1]))
            outs[-1].start()
        do[:, now] = dot_cols(wo[...], held[now, :]).astype(BF16)
        for i in range(first, done):
            outs.append(pltpu.make_async_copy(do.at[:, here(i)], do_hbm.at[:, there(i)], o_sem.at[i]))
            outs[-1].start()
        if low == 0 and gwo_load is not None:
            gwo_load.wait()
        share = jnp.dot(ot[:, now], held[now, :], preferred_element_type=F32)
        gwo[...] = share if begins and low == 0 else gwo[...] + share
    outs.append(pltpu.make_async_copy(gwo, gwo_hbm, o_sem.at[count]))
    outs[-1].start()
    for c in outs:
        c.wait()


def solution(mesh):
    n = mesh.shape["tp"]
    chips = n // 2
    right_of = [(i, ((i // 2 + 1) % chips) * 2 + i % 2) for i in range(n)]
    partner_of = [(i, i ^ 1) for i in range(n)]
    left_of = [(i, ((i // 2 - 1) % chips) * 2 + i % 2) for i in range(n)]

    def go_right(a):
        return lax.ppermute(a, "tp", right_of)

    def go_left(a):
        return lax.ppermute(a, "tp", left_of)

    def swap(a):
        return lax.ppermute(a, "tp", partner_of)

    token_spec = P(("dp", "tp"), None)
    split_cols = P("dp", "tp")
    weight_cols = P(None, "tp")
    weight_rows = P("tp", None)

    def run_main(x_norm, grad_y, u_gate_t, u_up_t, w_gate_t, w_up_t, w_down, x_in, gamma, grad_res):
        rows, hidden = x_norm.shape
        ffn, tokens = u_gate_t.shape
        half = rows // 2
        any_spec = pl.BlockSpec(memory_space=pl.ANY)
        dma = pltpu.SemaphoreType.DMA
        return pl.pallas_call(
            functools.partial(main_kernel, n),
            out_shape=[jax.ShapeDtypeStruct(*a) for a in (
                ((tokens, hidden), BF16), ((ffn, tokens), BF16), ((ffn, tokens), BF16),
                ((ffn, hidden), F32), ((ffn, hidden), F32), ((ffn, hidden), F32),
                *[((half // 2, hidden), BF16)] * 4, *[((half, hidden), BF16)] * 4)],
            in_specs=[any_spec] * 8 + [pl.BlockSpec(memory_space=pltpu.VMEM), any_spec],
            out_specs=[any_spec] * 14,
            scratch_shapes=[
                pltpu.VMEM((ffn, hidden), BF16), pltpu.VMEM((ffn, hidden), BF16), pltpu.VMEM((ffn, hidden), BF16),
                pltpu.VMEM((12, rows, hidden), BF16),
                pltpu.VMEM((2, ffn, rows), BF16), pltpu.VMEM((2, ffn, rows), BF16),
                pltpu.VMEM((ffn, rows), BF16), pltpu.VMEM((2, ffn, rows), BF16), pltpu.VMEM((2, ffn, rows), BF16),
                pltpu.VMEM((ffn, hidden), F32), pltpu.VMEM((4, rows, hidden), BF16),
                pltpu.VMEM((2, half, hidden), BF16), pltpu.VMEM((2, rows, hidden), BF16),
                dma((3,)), dma((2, 2)), dma((2, 4)), dma((2,)),
                dma((2, 3)), dma((4, 2)), dma((8, 2)),
                dma((2, 3)), dma((4, 2)), dma((8, 2)),
                dma((4,)), dma((4,)), dma((2,)), dma((2,)), dma((2, 2)), dma((2, 2)),
                dma((2, 4)), dma((2, 4)), dma((2, 4)), dma((2, 4)), dma((2, 4)),
                dma((2, 4)), dma((2, 4)),
            ],
            compiler_params=pltpu.CompilerParams(collective_id=0, has_side_effects=True,
                                                 vmem_limit_bytes=67_000_000),
        )(x_norm, grad_y, u_gate_t, u_up_t, w_gate_t, w_up_t, w_down, x_in, gamma, grad_res)

    any_space = pl.BlockSpec(memory_space=pl.ANY)

    def settle(*arrays):
        lines, hidden = arrays[0].shape
        slots = 10 * len(arrays)
        return pl.pallas_call(
            settle_kernel,
            in_specs=[any_space] * len(arrays), out_specs=[any_space] * len(arrays),
            out_shape=[jax.ShapeDtypeStruct(a.shape, a.dtype) for a in arrays],
            scratch_shapes=[pltpu.VMEM((slots, lines // 10, hidden), F32), pltpu.SemaphoreType.DMA((slots,)),
                            pltpu.SemaphoreType.DMA((slots,))],
            cost_estimate=pl.CostEstimate(flops=2000 * len(arrays) * lines * hidden,
                                          bytes_accessed=8 * len(arrays) * lines * hidden, transcendentals=0),
            compiler_params=pltpu.CompilerParams(vmem_limit_bytes=67_000_000),
        )(*arrays)

    def attn(pieces, rows, attn_t, w_out, *sofar):
        arrays, kinds = [p[0] for p in pieces], tuple(p[1:] for p in pieces)
        hidden, (width, tokens) = arrays[0].shape[1], attn_t.shape
        total, count = sum(a.shape[0] for a in arrays), len(arrays)
        dma = pltpu.SemaphoreType.DMA
        results = [jax.ShapeDtypeStruct((width, tokens), BF16), jax.ShapeDtypeStruct((width, hidden), F32)]
        if not sofar:
            results.insert(0, jax.ShapeDtypeStruct((rows, hidden), BF16))
        return pl.pallas_call(
            functools.partial(attn_kernel, n, kinds, rows),
            in_specs=[any_space] * (count + 2 + len(sofar)), out_specs=[any_space] * len(results),
            scratch_shapes=[
                pltpu.VMEM((total, hidden), BF16), pltpu.VMEM((width, total), BF16), pltpu.VMEM((width, hidden), BF16),
                pltpu.VMEM((width, total), BF16), pltpu.VMEM((width, hidden), F32),
                dma((count,)), dma((2 + count,)), dma((2 + count,))],
            out_shape=results,
            input_output_aliases={count + 3: 0} if sofar else {},
            cost_estimate=pl.CostEstimate(flops=1200 * total * hidden, bytes_accessed=8 * total * hidden,
                                          transcendentals=0),
            compiler_params=pltpu.CompilerParams(vmem_limit_bytes=67_000_000),
        )(*arrays, attn_t, w_out, *sofar)

    def local_backward(x_norm, grad_y, u_gate, u_up, w_gate, w_up, w_down, x_in, gamma, grad_res, attn_out, w_out):
        attn_t = attn_out.T
        rows = x_norm.shape[0]
        half, part = rows // 2, rows // 4
        (_, _, _, gate_t, up_t, down, top_a, top_b, low_a, low_b, other_top, other_low, left_top,
         right_low) = run_main(
            x_norm, grad_y, u_gate.T, u_up.T, w_gate.T, w_up.T, w_down, x_in, gamma, grad_res)

        def both(a, other, slot, row):
            return [(a, slot, 0, row), (other, slot, 1, row)]

        far_top, far_low = go_right(left_top), go_left(right_low)
        left_low_a, right_top_a = go_right(low_a), go_left(top_a)
        left_low_b, right_top_b = go_right(low_b), go_left(top_b)
        left_top_other, right_low_other = swap(left_top), swap(right_low)
        gate_t, up_t, gw_down = settle(gate_t, up_t, down)
        grad_sum, do_t, gwo = attn([
            (top_a, OWN, 0, 0), (top_b, OWN, 0, part), (low_a, OWN, 0, half), (low_b, OWN, 0, half + part),
            (other_top, OWN, 1, 0), (other_low, OWN, 1, half),
            *both(left_top, left_top_other, LEFT, 0), *both(right_low, right_low_other, RIGHT, half)],
            rows, attn_t, w_out)
        far_top_other, far_low_other = swap(far_top), swap(far_low)
        left_low_a_other, right_top_a_other = swap(left_low_a), swap(right_top_a)
        do_t, gwo = attn([
            *both(far_top, far_top_other, FAR, 0), *both(far_low, far_low_other, FAR, half),
            *both(left_low_a, left_low_a_other, LEFT, half), *both(right_top_a, right_top_a_other, RIGHT, 0)],
            rows, attn_t, w_out, gwo, do_t)
        left_low_b_other, right_top_b_other = swap(left_low_b), swap(right_top_b)
        do_t, gwo = attn([
            *both(left_low_b, left_low_b_other, LEFT, half + part),
            *both(right_top_b, right_top_b_other, RIGHT, part)], rows, attn_t, w_out, gwo, do_t)
        return grad_sum, do_t.T, gate_t.T, up_t.T, gw_down, gwo

    return jax.shard_map(
        local_backward,
        mesh=mesh,
        in_specs=(token_spec, token_spec, split_cols, split_cols, weight_cols, weight_cols, weight_rows,
                  token_spec, P(None), token_spec, split_cols, weight_rows),
        out_specs=(token_spec, split_cols, split_cols, split_cols, token_spec, token_spec),
        check_vma=False,
    )
```
